32 devices in a mesh: slab: 2 (over x), row: 8 (over z, y), col: 2 (over core).
Axes of the slice: x: 2, y: 2, z: 4, core: 2. Of those that a mesh axis runs over, the one named last changes fastest.
Arguments:
- image: float32 [1024, 4096], P(('slab', 'row'), 'col'), parts along dimension 0, may hold values from -6 to 6
Outputs:
- dog_fine: bfloat16 [4, 1024, 4096], P(None, ('slab', 'row'), 'col'), parts along dimension 1
- hessian_fine: bfloat16 [2, 1024, 4096], P(None, ('slab', 'row'), 'col'), parts along dimension 1
- dog_coarse: bfloat16 [4, 512, 2048], P(None, ('slab', 'row', 'col')), parts along dimension 1
- hessian_coarse: bfloat16 [2, 512, 2048], P(None, ('slab', 'row', 'col')), parts along dimension 1
The draws below stay inside these ranges and needn't reach their ends.
There are 2 independent parts, one for each index of `slab`. The reference program is written for one: setup_inputs(seed, part) draws one part's arguments, and reference() takes and returns one part's arrays. A program takes and returns all parts, laid end to end along the dimension named above; each array names one. Nothing has to cross between parts.
All inputs are finite; a program needn't handle non-finite values.
Results may differ from the reference program's by a relative error of at most 0.0013.
Values may be sent and summed in bfloat16 or wider, within the bound.
A program may use at most 64 MiB of HBM per device.

```python
import jax
import jax.numpy as jnp
from jax import lax

H = 512
W = 4096


def block_scale(rng, extent, split, low, largest):
    def one(dim, blocks):
        heights = jax.random.uniform(jax.random.fold_in(jax.random.fold_in(rng, 6), dim), (blocks,), jnp.float32, low / len(split), largest / len(split))
        return jnp.repeat(jnp.exp(heights), extent[dim] // blocks).reshape((-1,) + (1,) * (len(extent) - dim - 1))

    loudness = one(*split[0])
    for cut in split[1:]:
        loudness = loudness * one(*cut)
    return loudness


def normal_values(own_key, extent, scale, limit, cuts=(), kind=jnp.bfloat16):
    entries = jax.random.normal(own_key, extent, jnp.float32) * scale
    if len(cuts) > 0:
        entries = block_scale(own_key, extent, cuts, -0.22, 0.18) * entries
    return jnp.clip(entries, min=-limit, max=limit).astype(kind)


def setup_inputs(seed: int = 0, part: int = 0) -> dict:
    streams_of = jax.random.split(jax.random.key(seed), 2)
    part_splits = jax.random.split(jax.random.fold_in(streams_of[1], part), 2)
    return {
        "image": normal_values(part_splits[0], (H, W), 1.0, 6.0, ((0, 8), (1, 2)), jnp.float32),
    }


SIGMAS = [1.6 * 2.0 ** (k / 4.0) for k in range(5)]


def taps(sigma):
    offset = jnp.arange(25).astype(jnp.float32) - 12.0
    weights = jnp.exp(-offset * offset / (2.0 * sigma * sigma))
    return weights / jnp.sum(weights)


def blur(field, sigma):
    kernel = taps(sigma)
    data = field[None, None]
    vertical = lax.conv_general_dilated(data, kernel[None, None, :, None], (1, 1), ((12, 12), (0, 0)), precision=lax.Precision.HIGHEST)
    both = lax.conv_general_dilated(vertical, kernel[None, None, None, :], (1, 1), ((0, 0), (12, 12)), precision=lax.Precision.HIGHEST)
    return both[0, 0]


def hessian(diff):
    padded = jnp.pad(diff, 1)
    dxx = padded[1:-1, 2:] + padded[1:-1, :-2] - 2.0 * diff
    dyy = padded[2:, 1:-1] + padded[:-2, 1:-1] - 2.0 * diff
    dxy = (padded[2:, 2:] - padded[2:, :-2] - padded[:-2, 2:] + padded[:-2, :-2]) / 4.0
    return dxx * dyy - dxy * dxy


def octave(base, dog_gain, hess_gain):
    levels = [blur(base, s) for s in SIGMAS]
    diffs = [levels[k + 1] - levels[k] for k in range(4)]
    dogs = jnp.stack([(dog_gain * d).astype(jnp.bfloat16) for d in diffs])
    hess = jnp.stack([(hess_gain * hessian(diffs[m + 1])).astype(jnp.bfloat16) for m in range(2)])
    return dogs, hess, levels[4]


def reference(image):
    dog_fine, hessian_fine, top_level = octave(image, 20.0, 5000.0)
    coarse_base = top_level[0::2, 0::2]
    dog_coarse, hessian_coarse, unused = octave(coarse_base, 80.0, 200000.0)
    return dog_fine, hessian_fine, dog_coarse, hessian_coarse
```

```python
import functools

import jax
import jax.numpy as jnp
import numpy as np
from jax import lax
from jax.experimental import pallas as pl
from jax.experimental.pallas import tpu as pltpu
from jax.sharding import PartitionSpec as P

SIGMAS = [1.6 * 2.0 ** (k / 4.0) for k in range(5)]
LEVELS = 5
LANE = 128
HALF = LANE // 2
RIM = 16
CHUNK = 4
MESH = pl.DeviceIdType.MESH
BF = jnp.bfloat16
F32 = jnp.float32


def taps_at(sigma, offset):
    spread = np.arange(25, dtype=np.float64) - 12.0
    total = np.sum(np.exp(-spread * spread / (2.0 * sigma * sigma)))
    weight = np.exp(-(offset**2) / (2.0 * sigma * sigma)) / total
    return np.where(np.abs(offset) <= 12, weight, 0.0)


def halves(matrix):
    high = matrix.astype(BF)
    low = (matrix - high.astype(np.float64)).astype(BF)
    return high, low


def ring_rows(count):
    rows = np.full(count + 8, 10**6, dtype=np.float64)
    rows[: count + 1] = np.arange(count + 1)
    rows[-1] = -1
    return rows


def ring_inputs(count, before):
    total = np.arange(count, dtype=np.float64)
    return np.where(total >= count - before, total - count, total)


def vertical_matrix(out_rows, in_rows, sigma):
    return taps_at(sigma, in_rows[None, :] - out_rows[:, None])


def pad_rows(matrix, multiple):
    return np.pad(matrix, ((0, -matrix.shape[0] % multiple), (0, 0)))


def column_weights(matrix):
    high, low = halves(matrix)
    pair = np.concatenate([high, low], axis=1)
    return np.concatenate([pair, pair], axis=0)


def row_weights(matrix):
    high, low = halves(pad_rows(matrix, 16))
    return np.concatenate([high, high, low, low], axis=1)


def split(x):
    high = x.astype(BF)
    low = (x - high.astype(F32)).astype(BF)
    return high, low


def vertical_pass(source, matrix, vert, edge_keep, begin, end):
    tiles = source.shape[1] // LANE - 1
    lane = lax.broadcasted_iota(jnp.int32, (1, LANE), 1)

    def tile_of(t):
        value = source[:, t * LANE : (t + 1) * LANE]
        if t == tiles:
            value = value * edge_keep
        return pltpu.roll(value, HALF, 1)

    rolled = {t: tile_of(t % (tiles + 1)) for t in range(begin - 1, end)}
    left = lane < HALF
    group = [jnp.where(left, rolled[t - 1], rolled[t]) for t in range(begin, end)]
    high, low = split(jnp.concatenate(group, axis=1))
    stacked = jnp.concatenate([high, low, high, low], axis=0)
    vert[pl.ds(0, matrix.shape[0]), begin * LANE : end * LANE] = jnp.dot(
        matrix[...], stacked, preferred_element_type=F32
    )

def horizontal_pass(vert, g_level, lev, start, high_rows, begin, end):
    tiles = vert.shape[1] // LANE - 1

    for k in range(LEVELS):
        rows = pl.ds(start + k * high_rows, high_rows)
        windows = []
        for b in range(begin, end):
            if b == tiles:
                windows.append(
                    jnp.concatenate([vert[rows, b * LANE : (b + 1) * LANE], vert[rows, 0:LANE]], axis=1)
                )
            else:
                windows.append(vert[rows, b * LANE : (b + 2) * LANE])
        high, low = split(jnp.concatenate(windows, axis=0))
        product = jnp.dot(
            jnp.concatenate([high, low], axis=1), g_level[k], preferred_element_type=F32
        )
        lev[k, pl.ds(begin * high_rows, (end - begin) * high_rows), :] = (
            product[:, :LANE] + product[:, LANE:]
        )


def responses(lev, diff, count, blocks, dog_gain, hess_gain, row_keep, edge_keep, dog, hess):
    tiles = dog.shape[2] // LANE
    lane = lax.broadcasted_iota(jnp.int32, (1, LANE), 1)

    high_rows = count + 8
    for b in range(blocks):
        rows = pl.ds(b * high_rows, high_rows)
        level = [lev[k, rows, :] for k in range(LEVELS)]
        for k in range(LEVELS - 1):
            d = level[k + 1] - level[k]
            if b < tiles:
                dog[k, :, b * LANE : (b + 1) * LANE] = (dog_gain * d[:count]).astype(BF)
            if k in (1, 2):
                d = d * row_keep
                if b == tiles:
                    d = d * edge_keep
                diff[k - 1, rows, :] = d
    if blocks == tiles:
        diff[:, pl.ds(tiles * high_rows, high_rows), :] = jnp.zeros((2, high_rows, LANE), F32)

    def block(b):
        before, after = (b - 1) % (tiles + 1), (b + 1) % (tiles + 1)
        for m in range(2):
            centre = diff[m, pl.ds(b * high_rows, high_rows), :]
            previous = diff[m, pl.ds(before * high_rows, high_rows), :]
            following = diff[m, pl.ds(after * high_rows, high_rows), :]
            right = pltpu.roll(jnp.where(lane == 0, following, centre), LANE - 1, 1)
            left = pltpu.roll(jnp.where(lane == LANE - 1, previous, centre), 1, 1)
            slope = right - left
            dxx = (right + left - 2.0 * centre)[:count]
            twice = 2.0 * centre
            dyy = (
                pltpu.roll(centre, high_rows - 1, 0) + pltpu.roll(centre, 1, 0) - twice
            )[:count]
            dxy = (pltpu.roll(slope, high_rows - 1, 0) - pltpu.roll(slope, 1, 0))[:count] * 0.25
            hess[m, :, b * LANE : (b + 1) * LANE] = (hess_gain * (dxx * dyy - dxy * dxy)).astype(BF)

    for b in range(tiles):
        block(b)

def row_mask(count, before, after):
    index = lax.broadcasted_iota(jnp.int32, (count + 8, 1), 0)
    gone = jnp.logical_or(
        jnp.logical_and(index == count, jnp.logical_not(after)),
        jnp.logical_and(index == count + 7, jnp.logical_not(before)),
    )
    return jnp.where(gone, 0.0, 1.0).astype(F32)


def kernel(
    rows_total, image, a_fine_far, a_coarse_far, g_level_far, g_base_far,
    dog_fine, hess_fine, cext, a_coarse, g_level,
    ext, vert, lev, diff, base, a_fine, g_base,
    load_sem, fsend, frecv, csend, crecv,
):
    tile_rows, tile_cols = image.shape
    tiles = tile_cols // LANE
    strip = tile_rows // 4
    half_cols = tile_cols // 2
    r = lax.axis_index("row")
    c = lax.axis_index("col")
    other = 1 - c
    has_up = r > 0
    has_down = r < rows_total - 1

    load = pltpu.make_async_copy(image, ext.at[pl.ds(0, tile_rows), pl.ds(0, tile_cols)], load_sem.at[0])
    load.start()
    pairs = [(a_fine_far, a_fine), (g_base_far, g_base), (g_level_far, g_level), (a_coarse_far, a_coarse)]
    weights = [
        pltpu.make_async_copy(far, near, load_sem.at[1 + i]) for i, (far, near) in enumerate(pairs)
    ]

    barrier = pltpu.get_barrier_semaphore()

    def greet(row, col):
        pl.semaphore_signal(barrier, inc=1, device_id={"row": row, "col": col}, device_id_type=MESH)

    greet(r, other)

    @pl.when(has_up)
    def _():
        greet(r - 1, c)
        greet(r - 1, other)

    @pl.when(has_down)
    def _():
        greet(r + 1, c)
        greet(r + 1, other)

    ends = (r == 0).astype(jnp.int32) + (r == rows_total - 1).astype(jnp.int32)
    pl.semaphore_wait(barrier, 5 - 2 * ends)

    for weight in weights:
        weight.start()
    load.wait()

    def remote(src, dst, send, recv, row, col):
        return pltpu.make_async_remote_copy(
            src_ref=src, dst_ref=dst, send_sem=send, recv_sem=recv,
            device_id={"row": row, "col": col}, device_id_type=MESH,
        )

    edge = pl.ds(pl.multiple_of(other * (tile_cols - LANE), LANE), LANE)
    own = pl.ds(0, tile_cols)
    rim = pl.ds(tile_cols, LANE)
    first = pl.ds(0, RIM)
    last = pl.ds(tile_rows - RIM, RIM)
    below = pl.ds(tile_rows, RIM)
    above = pl.ds(tile_rows + RIM, RIM)
    inner = pl.ds(0, tile_rows)

    chunks = tiles // CHUNK
    span = CHUNK * LANE
    to_down, to_up = [], []
    for j in range(chunks):
        part = pl.ds(j * span, span)
        to_down.append(remote(ext.at[last, part], ext.at[above, part], fsend.at[2 * j], frecv.at[2 * j], r + 1, c))
        to_up.append(
            remote(ext.at[first, part], ext.at[below, part], fsend.at[2 * j + 1], frecv.at[2 * j + 1], r - 1, c)
        )
    n = 2 * chunks
    to_down_corner = remote(ext.at[last, edge], ext.at[above, rim], fsend.at[n], frecv.at[n], r + 1, other)
    to_up_corner = remote(ext.at[first, edge], ext.at[below, rim], fsend.at[n + 1], frecv.at[n + 1], r - 1, other)
    to_side = remote(ext.at[inner, edge], ext.at[inner, rim], fsend.at[n + 2], frecv.at[n + 2], r, other)

    @pl.when(has_down)
    def _():
        to_down_corner.start()
        to_down[0].start()

    @pl.when(has_up)
    def _():
        to_up_corner.start()
        for send in to_up:
            send.start()

    @pl.when(has_down)
    def _():
        for send in to_down[1:]:
            send.start()

    to_side.start()

    wide = tile_cols + LANE

    @pl.when(r == 0)
    def _():
        ext[above, :] = jnp.zeros((RIM, wide), F32)

    @pl.when(r == rows_total - 1)
    def _():
        ext[below, :] = jnp.zeros((RIM, wide), F32)

    cext[:, pl.ds(tile_cols, LANE)] = jnp.zeros((3 * strip, LANE), F32)

    @pl.when(jnp.logical_and(r == 0, c == 0))
    def _():
        cext[pl.ds(2 * strip, strip), own] = jnp.zeros((strip, tile_cols), F32)

    @pl.when(jnp.logical_and(r == rows_total - 1, c == 1))
    def _():
        cext[pl.ds(strip, strip), own] = jnp.zeros((strip, tile_cols), F32)

    for weight in weights:
        weight.wait()
    to_side.wait()

    @pl.when(has_up)
    def _():
        to_down_corner.wait_recv()

    @pl.when(has_down)
    def _():
        to_up_corner.wait_recv()

    lane = lax.broadcasted_iota(jnp.int32, (1, LANE), 1)

    half_rows = tile_rows // 2

    def base_pass(begin, end):
        windows = [vert[0:half_rows, 2 * b * LANE : (2 * b + 3) * LANE] for b in range(begin, end)]
        high, low = split(jnp.concatenate(windows, axis=0))
        product = jnp.dot(
            jnp.concatenate([high, low], axis=1), g_base[...], preferred_element_type=F32
        )
        product = product[:, :LANE] + product[:, LANE:]
        for b in range(begin, end):
            base[:, b * LANE : (b + 1) * LANE] = product[
                (b - begin) * half_rows : (b - begin + 1) * half_rows
            ]

    keep = jnp.where((lane < HALF) == (c == 0), 1.0, 0.0).astype(F32)
    sends, ups, downs = [], [], []
    base_done = 0
    blocks_done = 0
    for j in range(chunks):

        @pl.when(has_up)
        def _():
            to_down[j].wait_recv()

        @pl.when(has_down)
        def _():
            to_up[j].wait_recv()

        ready = CHUNK * (j + 1) + (1 if j == chunks - 1 else 0)
        vertical_pass(ext, a_fine, vert, keep, CHUNK * j, ready)
        base_end = (ready - 1) // 2
        base_pass(base_done, base_end)

        near = pl.ds(base_done * LANE, (base_end - base_done) * LANE)
        mine = pl.ds(
            pl.multiple_of(c * half_cols + base_done * LANE, LANE), (base_end - base_done) * LANE
        )
        top, bottom = base.at[pl.ds(0, strip), near], base.at[pl.ds(strip, strip), near]

        def slot_rows(index):
            return pl.ds(pl.multiple_of(index * strip, 8), strip)

        pair = [
            remote(top, cext.at[slot_rows(2 * other), mine], csend.at[4 * j], crecv.at[4 * j], r, other),
            remote(bottom, cext.at[slot_rows(c), mine], csend.at[4 * j + 1], crecv.at[4 * j + 1], r, other),
        ]
        up = remote(top, cext.at[slot_rows(1), mine], csend.at[4 * j + 2], crecv.at[4 * j + 2 + c], r - 1, 1)
        down = remote(bottom, cext.at[slot_rows(2), mine], csend.at[4 * j + 3], crecv.at[4 * j + 2 + c], r + 1, 0)
        sends += pair
        ups.append(up)
        downs.append(down)

        @pl.when(has_up)
        def _():
            up.start()

        @pl.when(has_down)
        def _():
            down.start()

        for send in pair:
            send.start()

        cext[slot_rows(2 * c), mine] = base[0:strip, near]
        cext[slot_rows(other), mine] = base[strip : 2 * strip, near]

        blocks_end = tiles + 1 if j == chunks - 1 else ready - 1
        horizontal_pass(vert, g_level, lev, half_rows, tile_rows + 8, blocks_done, blocks_end)
        base_done, blocks_done = base_end, blocks_end

    edge_keep = jnp.where(lane == jnp.where(c == 0, 0, LANE - 1), 1.0, 0.0).astype(F32)
    responses(
        lev, diff, tile_rows, tiles + 1, 20.0, 5000.0,
        row_mask(tile_rows, has_up, has_down), edge_keep, dog_fine, hess_fine,
    )

    for send in sends:
        send.wait_recv()

    @pl.when(jnp.logical_or(c == 1, has_up))
    def _():
        @pl.when(jnp.logical_or(c == 0, has_down))
        def _():
            for j in range(chunks):
                for index in range(2):
                    pltpu.make_async_remote_copy(
                        src_ref=ups[j].src_ref, dst_ref=ups[j].dst_ref,
                        send_sem=csend.at[4 * j + 2], recv_sem=crecv.at[4 * j + 2 + index],
                        device_id={"row": r, "col": other}, device_id_type=MESH,
                    ).wait_recv()

    @pl.when(has_down)
    def _():
        to_down_corner.wait_send()
        for send in to_down + downs:
            send.wait_send()

    @pl.when(has_up)
    def _():
        to_up_corner.wait_send()
        for send in to_up + ups:
            send.wait_send()

    for send in sends:
        send.wait_send()


def finish(
    rows_total, dog_near, hess_near, cext, a_coarse, g_level,
    dog_fine, hess_fine, dog_coarse, hess_coarse,
    vert, lev, diff, dog, hess, sem,
):
    strip = cext.shape[0] // 3
    tiles = cext.shape[1] // LANE - 1
    r = lax.axis_index("row")
    c = lax.axis_index("col")
    fine = [
        pltpu.make_async_copy(dog_near, dog_fine, sem.at[0]),
        pltpu.make_async_copy(hess_near, hess_fine, sem.at[1]),
    ]
    for copy in fine:
        copy.start()
    for begin in range(0, tiles, CHUNK):
        end = begin + CHUNK + (1 if begin + CHUNK == tiles else 0)
        vertical_pass(cext, a_coarse, vert, jnp.ones((1, LANE), F32), begin, end)
    horizontal_pass(vert, g_level, lev, 0, strip + 8, 0, tiles)
    responses(
        lev, diff, strip, tiles, 80.0, 200000.0,
        row_mask(strip, jnp.logical_or(r > 0, c == 1), jnp.logical_or(r < rows_total - 1, c == 0)),
        None, dog, hess,
    )
    coarse = [
        pltpu.make_async_copy(dog, dog_coarse, sem.at[2]),
        pltpu.make_async_copy(hess, hess_coarse, sem.at[3]),
    ]
    for copy in coarse:
        copy.start()
    for copy in fine + coarse:
        copy.wait()


def solution(mesh):
    rows_total = mesh.shape["row"]

    def local(image):
        tile_rows, tile_cols = image.shape
        strip = tile_rows // 4
        tiles = tile_cols // LANE
        fine_in = ring_inputs(tile_rows + 2 * RIM, RIM)
        coarse_in = ring_inputs(3 * strip, strip)
        a_fine = row_weights(
            np.concatenate(
                [vertical_matrix(2.0 * np.arange(tile_rows // 2), fine_in, SIGMAS[4])]
                + [vertical_matrix(ring_rows(tile_rows), fine_in, s) for s in SIGMAS]
            )
        )
        a_coarse = row_weights(
            np.concatenate([vertical_matrix(ring_rows(strip), coarse_in, s) for s in SIGMAS])
        )
        window = np.arange(2 * LANE, dtype=np.float64)[:, None] - HALF
        g_level = np.stack(
            [column_weights(taps_at(s, window - np.arange(LANE)[None, :])) for s in SIGMAS]
        )
        wider = np.arange(3 * LANE, dtype=np.float64)[:, None] - HALF
        g_base = column_weights(taps_at(SIGMAS[4], wider - 2.0 * np.arange(LANE)[None, :]))

        vmem = pl.BlockSpec(memory_space=pltpu.VMEM)
        ring = tile_rows + 8
        wide = tile_cols + LANE
        chunks = tiles // CHUNK
        hbm = pl.BlockSpec(memory_space=pltpu.HBM)
        near = pl.pallas_call(
            functools.partial(kernel, rows_total),
            out_shape=(
                pltpu.VMEM((4, tile_rows, tile_cols), BF),
                pltpu.VMEM((2, tile_rows, tile_cols), BF),
                pltpu.VMEM((3 * strip, wide), F32),
                pltpu.VMEM(a_coarse.shape, BF),
                pltpu.VMEM(g_level.shape, BF),
            ),
            in_specs=[hbm] * 5,
            out_specs=(vmem,) * 5,
            scratch_shapes=[
                pltpu.VMEM((tile_rows + 2 * RIM, wide), F32),
                pltpu.VMEM((a_fine.shape[0], wide), F32),
                pltpu.VMEM((LEVELS, (tiles + 1) * ring, LANE), F32),
                pltpu.VMEM((2, (tiles + 1) * ring, LANE), F32),
                pltpu.VMEM((tile_rows // 2, tile_cols // 2), F32),
                pltpu.VMEM(a_fine.shape, BF),
                pltpu.VMEM(g_base.shape, BF),
                pltpu.SemaphoreType.DMA((5,)),
                pltpu.SemaphoreType.DMA((2 * chunks + 3,)),
                pltpu.SemaphoreType.DMA((2 * chunks + 3,)),
                pltpu.SemaphoreType.DMA((4 * chunks,)),
                pltpu.SemaphoreType.DMA((4 * chunks,)),
            ],
            compiler_params=pltpu.CompilerParams(
                collective_id=0, has_side_effects=True, vmem_limit_bytes=32000000
            ),
        )(*[pltpu.with_memory_space_constraint(x, pltpu.HBM) for x in (image, a_fine, a_coarse, g_level, g_base)])
        coarse_ring = strip + 8
        return pl.pallas_call(
            functools.partial(finish, rows_total),
            out_shape=(
                jax.ShapeDtypeStruct((4, tile_rows, tile_cols), BF),
                jax.ShapeDtypeStruct((2, tile_rows, tile_cols), BF),
                jax.ShapeDtypeStruct((4, strip, tile_cols), BF),
                jax.ShapeDtypeStruct((2, strip, tile_cols), BF),
            ),
            in_specs=[vmem] * 5,
            out_specs=(hbm,) * 4,
            scratch_shapes=[
                pltpu.VMEM((a_coarse.shape[0], wide), F32),
                pltpu.VMEM((LEVELS, tiles * coarse_ring, LANE), F32),
                pltpu.VMEM((2, (tiles + 1) * coarse_ring, LANE), F32),
                pltpu.VMEM((4, strip, tile_cols), BF),
                pltpu.VMEM((2, strip, tile_cols), BF),
                pltpu.SemaphoreType.DMA((4,)),
            ],
            compiler_params=pltpu.CompilerParams(vmem_limit_bytes=32000000),
        )(*near)

    return jax.shard_map(
        local,
        mesh=mesh,
        in_specs=(P(("slab", "row"), "col"),),
        out_specs=(
            P(None, ("slab", "row"), "col"),
            P(None, ("slab", "row"), "col"),
            P(None, ("slab", "row", "col"), None),
            P(None, ("slab", "row", "col"), None),
        ),
        check_vma=False,
    )
```

```python
import functools

import jax
import jax.numpy as jnp
import numpy as np
from jax import lax
from jax.experimental import pallas as pl
from jax.experimental.pallas import tpu as pltpu
from jax.sharding import PartitionSpec as P

SIGMAS = [1.6 * 2.0 ** (k / 4.0) for k in range(5)]
LEVELS = 5
LANE = 128
HALF = LANE // 2
RIM = 16
NEED = 13
SPARE = RIM - NEED
CHUNK = 4
MESH = pl.DeviceIdType.MESH
BF = jnp.bfloat16
F32 = jnp.float32


def taps_at(sigma, offset):
    spread = np.arange(25, dtype=np.float64) - 12.0
    total = np.sum(np.exp(-spread * spread / (2.0 * sigma * sigma)))
    weight = np.exp(-(offset**2) / (2.0 * sigma * sigma)) / total
    return np.where(np.abs(offset) <= 12, weight, 0.0)


def halves(matrix):
    high = matrix.astype(BF)
    low = (matrix - high.astype(np.float64)).astype(BF)
    return high, low


def ring_rows(count):
    rows = np.full(count + 8, 10**6, dtype=np.float64)
    rows[: count + 1] = np.arange(count + 1)
    rows[-1] = -1
    return rows


def ring_inputs(count, before):
    total = np.arange(count, dtype=np.float64)
    return np.where(total >= count - before, total - count, total)


def vertical_matrix(out_rows, in_rows, sigma):
    return taps_at(sigma, in_rows[None, :] - out_rows[:, None])


def pad_rows(matrix, multiple):
    return np.pad(matrix, ((0, -matrix.shape[0] % multiple), (0, 0)))


def column_weights(matrix):
    high, low = halves(matrix)
    pair = np.concatenate([high, low], axis=1)
    return np.concatenate([pair, pair], axis=0)


def rim_inputs(count):
    slot = np.arange(RIM, dtype=np.float64)
    above = np.where(slot >= SPARE, slot - RIM, slot - SPARE)
    below = count + np.where(slot < NEED, slot, slot - NEED)
    return np.concatenate([above, below])


def fine_weights(own, rim):
    high, low = halves(pad_rows(own, 16))
    rim_high, rim_low = halves(pad_rows(rim, 16))
    return np.concatenate([high, high, low, rim_high, rim_low], axis=1)


def row_weights(matrix):
    high, low = halves(pad_rows(matrix, 16))
    return np.concatenate([high, high, low, low], axis=1)


def split(x):
    high = x.astype(BF)
    low = (x - high.astype(F32)).astype(BF)
    return high, low


def packed(x, shift, keep_high):
    high = x.astype(BF).astype(F32)
    return jnp.where(keep_high, high, pltpu.roll(x - high, shift, 0)).astype(BF)


def fine_vertical_pass(ext, rim, matrix, vert, edge_keep, begin, end):
    tiles = ext.shape[1] // LANE - 1
    left = lax.broadcasted_iota(jnp.int32, (1, LANE), 1) < HALF

    def tile_of(t):
        part = slice(t * LANE, (t + 1) * LANE)
        value = jnp.concatenate([ext[:, part], rim[0, :, part].astype(F32), rim[1, :, part].astype(F32)], axis=0)
        if t == tiles:
            value = value * edge_keep
        return pltpu.roll(value, HALF, 1)

    rows = ext.shape[0]
    rolled = {t: tile_of(t % (tiles + 1)) for t in range(begin - 1, end)}
    group = jnp.concatenate([jnp.where(left, rolled[t - 1], rolled[t]) for t in range(begin, end)], axis=1)
    high, low = split(group[:rows])
    edges = group[rows:].astype(BF)
    stacked = jnp.concatenate([high, low, high, edges, edges], axis=0)
    vert[pl.ds(0, matrix.shape[0]), begin * LANE : end * LANE] = jnp.dot(
        matrix[...], stacked, preferred_element_type=F32
    )


def vertical_pass(source, matrix, vert, edge_keep, begin, end):
    tiles = source.shape[1] // LANE - 1
    lane = lax.broadcasted_iota(jnp.int32, (1, LANE), 1)

    def tile_of(t):
        value = source[:, t * LANE : (t + 1) * LANE]
        if t == tiles:
            value = value * edge_keep
        return pltpu.roll(value, HALF, 1)

    rolled = {t: tile_of(t % (tiles + 1)) for t in range(begin - 1, end)}
    left = lane < HALF
    group = [jnp.where(left, rolled[t - 1], rolled[t]) for t in range(begin, end)]
    high, low = split(jnp.concatenate(group, axis=1))
    stacked = jnp.concatenate([high, low, high, low], axis=0)
    vert[pl.ds(0, matrix.shape[0]), begin * LANE : end * LANE] = jnp.dot(
        matrix[...], stacked, preferred_element_type=F32
    )

def horizontal_pass(vert, g_level, lev, start, high_rows, begin, end):
    tiles = vert.shape[1] // LANE - 1

    for k in range(LEVELS):
        rows = pl.ds(start + k * high_rows, high_rows)
        windows = []
        for b in range(begin, end):
            if b == tiles:
                windows.append(
                    jnp.concatenate([vert[rows, b * LANE : (b + 1) * LANE], vert[rows, 0:LANE]], axis=1)
                )
            else:
                windows.append(vert[rows, b * LANE : (b + 2) * LANE])
        high, low = split(jnp.concatenate(windows, axis=0))
        product = jnp.dot(
            jnp.concatenate([high, low], axis=1), g_level[k], preferred_element_type=F32
        )
        lev[k, pl.ds(begin * high_rows, (end - begin) * high_rows), :] = (
            product[:, :LANE] + product[:, LANE:]
        )


def responses(lev, diff, count, blocks, dog_gain, hess_gain, row_keep, edge_keep, dog, hess):
    tiles = dog.shape[2] // LANE
    lane = lax.broadcasted_iota(jnp.int32, (1, LANE), 1)

    high_rows = count + 8
    for b in range(blocks):
        rows = pl.ds(b * high_rows, high_rows)
        level = [lev[k, rows, :] for k in range(LEVELS)]
        for k in range(LEVELS - 1):
            d = level[k + 1] - level[k]
            if b < tiles:
                dog[k, :, b * LANE : (b + 1) * LANE] = (dog_gain * d[:count]).astype(BF)
            if k in (1, 2):
                d = d * row_keep
                if b == tiles:
                    d = d * edge_keep
                diff[k - 1, rows, :] = d
    if blocks == tiles:
        diff[:, pl.ds(tiles * high_rows, high_rows), :] = jnp.zeros((2, high_rows, LANE), F32)

    def block(b):
        before, after = (b - 1) % (tiles + 1), (b + 1) % (tiles + 1)
        for m in range(2):
            centre = diff[m, pl.ds(b * high_rows, high_rows), :]
            previous = diff[m, pl.ds(before * high_rows, high_rows), :]
            following = diff[m, pl.ds(after * high_rows, high_rows), :]
            right = pltpu.roll(jnp.where(lane == 0, following, centre), LANE - 1, 1)
            left = pltpu.roll(jnp.where(lane == LANE - 1, previous, centre), 1, 1)
            slope = right - left
            dxx = (right + left - 2.0 * centre)[:count]
            twice = 2.0 * centre
            dyy = (
                pltpu.roll(centre, high_rows - 1, 0) + pltpu.roll(centre, 1, 0) - twice
            )[:count]
            dxy = (pltpu.roll(slope, high_rows - 1, 0) - pltpu.roll(slope, 1, 0))[:count] * 0.25
            hess[m, :, b * LANE : (b + 1) * LANE] = (hess_gain * (dxx * dyy - dxy * dxy)).astype(BF)

    for b in range(tiles):
        block(b)

def row_mask(count, before, after):
    index = lax.broadcasted_iota(jnp.int32, (count + 8, 1), 0)
    gone = jnp.logical_or(
        jnp.logical_and(index == count, jnp.logical_not(after)),
        jnp.logical_and(index == count + 7, jnp.logical_not(before)),
    )
    return jnp.where(gone, 0.0, 1.0).astype(F32)


def kernel(
    rows_total, image, a_fine_far, a_coarse_far, g_level_far, g_base_far,
    dog_fine, hess_fine, cext, a_coarse, g_level,
    ext, rim_out, rim_in, vert, lev, diff, base, a_fine, g_base,
    load_sem, fsend, frecv, csend, crecv,
):
    tile_rows, tile_cols = image.shape
    tiles = tile_cols // LANE
    strip = tile_rows // 4
    half_cols = tile_cols // 2
    r = lax.axis_index("row")
    c = lax.axis_index("col")
    other = 1 - c
    has_up = r > 0
    has_down = r < rows_total - 1

    load = pltpu.make_async_copy(image, ext.at[pl.ds(0, tile_rows), pl.ds(0, tile_cols)], load_sem.at[0])
    load.start()
    pairs = [(a_fine_far, a_fine), (g_base_far, g_base), (g_level_far, g_level), (a_coarse_far, a_coarse)]
    weights = [
        pltpu.make_async_copy(far, near, load_sem.at[1 + i]) for i, (far, near) in enumerate(pairs)
    ]

    barrier = pltpu.get_barrier_semaphore()

    def greet(row, col):
        pl.semaphore_signal(barrier, inc=1, device_id={"row": row, "col": col}, device_id_type=MESH)

    greet(r, other)

    @pl.when(has_up)
    def _():
        greet(r - 1, c)
        greet(r - 1, other)

    @pl.when(has_down)
    def _():
        greet(r + 1, c)
        greet(r + 1, other)

    for weight in weights:
        weight.start()
    load.wait()

    slot = lax.broadcasted_iota(jnp.int32, (RIM, 1), 0)

    def pack(j):
        part = slice(j * CHUNK * LANE, (j + 1) * CHUNK * LANE)
        rim_out[0, :, part] = packed(ext[0:RIM, part], NEED, slot < NEED)
        rim_out[1, :, part] = packed(ext[tile_rows - RIM : tile_rows, part], SPARE, slot >= SPARE)

    for j in range(tiles // CHUNK):
        pack(j)

    ends = (r == 0).astype(jnp.int32) + (r == rows_total - 1).astype(jnp.int32)
    pl.semaphore_wait(barrier, 5 - 2 * ends)

    def remote(src, dst, send, recv, row, col):
        return pltpu.make_async_remote_copy(
            src_ref=src, dst_ref=dst, send_sem=send, recv_sem=recv,
            device_id={"row": row, "col": col}, device_id_type=MESH,
        )

    edge = pl.ds(pl.multiple_of(other * (tile_cols - LANE), LANE), LANE)
    own = pl.ds(0, tile_cols)
    rim = pl.ds(tile_cols, LANE)
    inner = pl.ds(0, tile_rows)
    first, last, above, below = rim_out.at[0], rim_out.at[1], rim_in.at[0], rim_in.at[1]
    whole = pl.ds(0, RIM)

    chunks = tiles // CHUNK
    span = CHUNK * LANE
    to_down, to_up = [], []
    for j in range(chunks):
        part = pl.ds(j * span, span)
        to_down.append(remote(last.at[whole, part], above.at[whole, part], fsend.at[2 * j], frecv.at[2 * j], r + 1, c))
        to_up.append(
            remote(first.at[whole, part], below.at[whole, part], fsend.at[2 * j + 1], frecv.at[2 * j + 1], r - 1, c)
        )
    n = 2 * chunks
    to_down_corner = remote(last.at[whole, edge], above.at[whole, rim], fsend.at[n], frecv.at[n], r + 1, other)
    to_up_corner = remote(first.at[whole, edge], below.at[whole, rim], fsend.at[n + 1], frecv.at[n + 1], r - 1, other)
    to_side = remote(ext.at[inner, edge], ext.at[inner, rim], fsend.at[n + 2], frecv.at[n + 2], r, other)

    @pl.when(has_down)
    def _():
        to_down_corner.start()
        to_down[0].start()

    @pl.when(has_up)
    def _():
        to_up_corner.start()
        for send in to_up:
            send.start()

    @pl.when(has_down)
    def _():
        for send in to_down[1:]:
            send.start()

    to_side.start()

    wide = tile_cols + LANE

    @pl.when(r == 0)
    def _():
        rim_in[0, :, :] = jnp.zeros((RIM, wide), BF)

    @pl.when(r == rows_total - 1)
    def _():
        rim_in[1, :, :] = jnp.zeros((RIM, wide), BF)

    cext[:, pl.ds(tile_cols, LANE)] = jnp.zeros((3 * strip, LANE), F32)

    @pl.when(jnp.logical_and(r == 0, c == 0))
    def _():
        cext[pl.ds(2 * strip, strip), own] = jnp.zeros((strip, tile_cols), F32)

    @pl.when(jnp.logical_and(r == rows_total - 1, c == 1))
    def _():
        cext[pl.ds(strip, strip), own] = jnp.zeros((strip, tile_cols), F32)

    for weight in weights:
        weight.wait()
    to_side.wait()

    @pl.when(has_up)
    def _():
        to_down_corner.wait_recv()

    @pl.when(has_down)
    def _():
        to_up_corner.wait_recv()

    lane = lax.broadcasted_iota(jnp.int32, (1, LANE), 1)

    half_rows = tile_rows // 2

    def base_pass(begin, end):
        windows = [vert[0:half_rows, 2 * b * LANE : (2 * b + 3) * LANE] for b in range(begin, end)]
        high, low = split(jnp.concatenate(windows, axis=0))
        product = jnp.dot(
            jnp.concatenate([high, low], axis=1), g_base[...], preferred_element_type=F32
        )
        product = product[:, :LANE] + product[:, LANE:]
        for b in range(begin, end):
            base[:, b * LANE : (b + 1) * LANE] = product[
                (b - begin) * half_rows : (b - begin + 1) * half_rows
            ]

    keep = jnp.where((lane < HALF) == (c == 0), 1.0, 0.0).astype(F32)
    sends, ups, downs = [], [], []
    base_done = 0
    blocks_done = 0
    for j in range(chunks):

        @pl.when(has_up)
        def _():
            to_down[j].wait_recv()

        @pl.when(has_down)
        def _():
            to_up[j].wait_recv()

        ready = CHUNK * (j + 1) + (1 if j == chunks - 1 else 0)
        fine_vertical_pass(ext, rim_in, a_fine, vert, keep, CHUNK * j, ready)
        base_end = (ready - 1) // 2
        base_pass(base_done, base_end)

        near = pl.ds(base_done * LANE, (base_end - base_done) * LANE)
        mine = pl.ds(
            pl.multiple_of(c * half_cols + base_done * LANE, LANE), (base_end - base_done) * LANE
        )
        top, bottom = base.at[pl.ds(0, strip), near], base.at[pl.ds(strip, strip), near]

        def slot_rows(index):
            return pl.ds(pl.multiple_of(index * strip, 8), strip)

        pair = [
            remote(top, cext.at[slot_rows(2 * other), mine], csend.at[4 * j], crecv.at[4 * j], r, other),
            remote(bottom, cext.at[slot_rows(c), mine], csend.at[4 * j + 1], crecv.at[4 * j + 1], r, other),
        ]
        up = remote(top, cext.at[slot_rows(1), mine], csend.at[4 * j + 2], crecv.at[4 * j + 2 + c], r - 1, 1)
        down = remote(bottom, cext.at[slot_rows(2), mine], csend.at[4 * j + 3], crecv.at[4 * j + 2 + c], r + 1, 0)
        sends += pair
        ups.append(up)
        downs.append(down)

        @pl.when(has_up)
        def _():
            up.start()

        @pl.when(has_down)
        def _():
            down.start()

        for send in pair:
            send.start()

        cext[slot_rows(2 * c), mine] = base[0:strip, near]
        cext[slot_rows(other), mine] = base[strip : 2 * strip, near]

        blocks_end = tiles + 1 if j == chunks - 1 else ready - 1
        horizontal_pass(vert, g_level, lev, half_rows, tile_rows + 8, blocks_done, blocks_end)
        base_done, blocks_done = base_end, blocks_end

    edge_keep = jnp.where(lane == jnp.where(c == 0, 0, LANE - 1), 1.0, 0.0).astype(F32)
    responses(
        lev, diff, tile_rows, tiles + 1, 20.0, 5000.0,
        row_mask(tile_rows, has_up, has_down), edge_keep, dog_fine, hess_fine,
    )

    for send in sends:
        send.wait_recv()

    @pl.when(jnp.logical_or(c == 1, has_up))
    def _():
        @pl.when(jnp.logical_or(c == 0, has_down))
        def _():
            for j in range(chunks):
                for index in range(2):
                    pltpu.make_async_remote_copy(
                        src_ref=ups[j].src_ref, dst_ref=ups[j].dst_ref,
                        send_sem=csend.at[4 * j + 2], recv_sem=crecv.at[4 * j + 2 + index],
                        device_id={"row": r, "col": other}, device_id_type=MESH,
                    ).wait_recv()

    @pl.when(has_down)
    def _():
        to_down_corner.wait_send()
        for send in to_down + downs:
            send.wait_send()

    @pl.when(has_up)
    def _():
        to_up_corner.wait_send()
        for send in to_up + ups:
            send.wait_send()

    for send in sends:
        send.wait_send()


def finish(
    rows_total, dog_near, hess_near, cext, a_coarse, g_level,
    dog_fine, hess_fine, dog_coarse, hess_coarse,
    vert, lev, diff, dog, hess, sem,
):
    strip = cext.shape[0] // 3
    tiles = cext.shape[1] // LANE - 1
    r = lax.axis_index("row")
    c = lax.axis_index("col")
    fine = [
        pltpu.make_async_copy(dog_near, dog_fine, sem.at[0]),
        pltpu.make_async_copy(hess_near, hess_fine, sem.at[1]),
    ]
    for copy in fine:
        copy.start()
    for begin in range(0, tiles, CHUNK):
        end = begin + CHUNK + (1 if begin + CHUNK == tiles else 0)
        vertical_pass(cext, a_coarse, vert, jnp.ones((1, LANE), F32), begin, end)
    horizontal_pass(vert, g_level, lev, 0, strip + 8, 0, tiles)
    responses(
        lev, diff, strip, tiles, 80.0, 200000.0,
        row_mask(strip, jnp.logical_or(r > 0, c == 1), jnp.logical_or(r < rows_total - 1, c == 0)),
        None, dog, hess,
    )
    coarse = [
        pltpu.make_async_copy(dog, dog_coarse, sem.at[2]),
        pltpu.make_async_copy(hess, hess_coarse, sem.at[3]),
    ]
    for copy in coarse:
        copy.start()
    for copy in fine + coarse:
        copy.wait()


def solution(mesh):
    rows_total = mesh.shape["row"]

    def local(image):
        tile_rows, tile_cols = image.shape
        strip = tile_rows // 4
        tiles = tile_cols // LANE
        coarse_in = ring_inputs(3 * strip, strip)
        fine_out = [(2.0 * np.arange(tile_rows // 2), SIGMAS[4])] + [(ring_rows(tile_rows), s) for s in SIGMAS]

        def fine_matrix(inputs):
            return np.concatenate([vertical_matrix(rows, inputs, s) for rows, s in fine_out])

        a_fine = fine_weights(
            fine_matrix(np.arange(tile_rows, dtype=np.float64)), fine_matrix(rim_inputs(tile_rows))
        )
        a_coarse = row_weights(
            np.concatenate([vertical_matrix(ring_rows(strip), coarse_in, s) for s in SIGMAS])
        )
        window = np.arange(2 * LANE, dtype=np.float64)[:, None] - HALF
        g_level = np.stack(
            [column_weights(taps_at(s, window - np.arange(LANE)[None, :])) for s in SIGMAS]
        )
        wider = np.arange(3 * LANE, dtype=np.float64)[:, None] - HALF
        g_base = column_weights(taps_at(SIGMAS[4], wider - 2.0 * np.arange(LANE)[None, :]))

        vmem = pl.BlockSpec(memory_space=pltpu.VMEM)
        ring = tile_rows + 8
        wide = tile_cols + LANE
        chunks = tiles // CHUNK
        hbm = pl.BlockSpec(memory_space=pltpu.HBM)
        near = pl.pallas_call(
            functools.partial(kernel, rows_total),
            out_shape=(
                pltpu.VMEM((4, tile_rows, tile_cols), BF),
                pltpu.VMEM((2, tile_rows, tile_cols), BF),
                pltpu.VMEM((3 * strip, wide), F32),
                pltpu.VMEM(a_coarse.shape, BF),
                pltpu.VMEM(g_level.shape, BF),
            ),
            in_specs=[hbm] * 5,
            out_specs=(vmem,) * 5,
            scratch_shapes=[
                pltpu.VMEM((tile_rows, wide), F32),
                pltpu.VMEM((2, RIM, tile_cols), BF),
                pltpu.VMEM((2, RIM, wide), BF),
                pltpu.VMEM((a_fine.shape[0], wide), F32),
                pltpu.VMEM((LEVELS, (tiles + 1) * ring, LANE), F32),
                pltpu.VMEM((2, (tiles + 1) * ring, LANE), F32),
                pltpu.VMEM((tile_rows // 2, tile_cols // 2), F32),
                pltpu.VMEM(a_fine.shape, BF),
                pltpu.VMEM(g_base.shape, BF),
                pltpu.SemaphoreType.DMA((5,)),
                pltpu.SemaphoreType.DMA((2 * chunks + 3,)),
                pltpu.SemaphoreType.DMA((2 * chunks + 3,)),
                pltpu.SemaphoreType.DMA((4 * chunks,)),
                pltpu.SemaphoreType.DMA((4 * chunks,)),
            ],
            compiler_params=pltpu.CompilerParams(
                collective_id=0, has_side_effects=True, vmem_limit_bytes=32000000
            ),
        )(*[pltpu.with_memory_space_constraint(x, pltpu.HBM) for x in (image, a_fine, a_coarse, g_level, g_base)])
        coarse_ring = strip + 8
        return pl.pallas_call(
            functools.partial(finish, rows_total),
            out_shape=(
                jax.ShapeDtypeStruct((4, tile_rows, tile_cols), BF),
                jax.ShapeDtypeStruct((2, tile_rows, tile_cols), BF),
                jax.ShapeDtypeStruct((4, strip, tile_cols), BF),
                jax.ShapeDtypeStruct((2, strip, tile_cols), BF),
            ),
            in_specs=[vmem] * 5,
            out_specs=(hbm,) * 4,
            scratch_shapes=[
                pltpu.VMEM((a_coarse.shape[0], wide), F32),
                pltpu.VMEM((LEVELS, tiles * coarse_ring, LANE), F32),
                pltpu.VMEM((2, (tiles + 1) * coarse_ring, LANE), F32),
                pltpu.VMEM((4, strip, tile_cols), BF),
                pltpu.VMEM((2, strip, tile_cols), BF),
                pltpu.SemaphoreType.DMA((4,)),
            ],
            compiler_params=pltpu.CompilerParams(vmem_limit_bytes=32000000),
        )(*near)

    return jax.shard_map(
        local,
        mesh=mesh,
        in_specs=(P(("slab", "row"), "col"),),
        out_specs=(
            P(None, ("slab", "row"), "col"),
            P(None, ("slab", "row"), "col"),
            P(None, ("slab", "row", "col"), None),
            P(None, ("slab", "row", "col"), None),
        ),
        check_vma=False,
    )
```

```python
import functools

import jax
import jax.numpy as jnp
import numpy as np
from jax import lax
from jax.experimental import pallas as pl
from jax.experimental.pallas import tpu as pltpu
from jax.sharding import PartitionSpec as P

SIGMAS = [1.6 * 2.0 ** (k / 4.0) for k in range(5)]
LEVELS = 5
LANE = 128
HALF = LANE // 2
RIM = 16
NEED = 13
SPARE = RIM - NEED
EDGE = 16
RING = 8
CHUNK = 4
MESH = pl.DeviceIdType.MESH
BF = jnp.bfloat16
F32 = jnp.float32


def taps_at(sigma, offset):
    spread = np.arange(25, dtype=np.float64) - 12.0
    total = np.sum(np.exp(-spread * spread / (2.0 * sigma * sigma)))
    weight = np.exp(-(offset**2) / (2.0 * sigma * sigma)) / total
    return np.where(np.abs(offset) <= 12, weight, 0.0)


def halves(matrix):
    high = matrix.astype(BF)
    low = (matrix - high.astype(np.float64)).astype(BF)
    return high, low


def ring_rows(count):
    rows = np.full(count + 8, 10**6, dtype=np.float64)
    rows[: count + 1] = np.arange(count + 1)
    rows[-1] = -1
    return rows


def vertical_matrix(out_rows, in_rows, sigma):
    return taps_at(sigma, in_rows[None, :] - out_rows[:, None])


def pad_rows(matrix, multiple):
    return np.pad(matrix, ((0, -matrix.shape[0] % multiple), (0, 0)))


def column_weights(matrix):
    high, low = halves(matrix)
    pair = np.concatenate([high, low], axis=1)
    return np.concatenate([pair, pair], axis=0)


def rim_inputs(count):
    slot = np.arange(RIM, dtype=np.float64)
    above = np.where(slot >= SPARE, slot - RIM, slot - SPARE)
    below = count + np.where(slot < NEED, slot, slot - NEED)
    return np.concatenate([above, below])


def own_weights(matrix):
    high, low = halves(matrix)
    return np.concatenate([high, high, low], axis=1)


def rim_weights(matrix):
    return np.concatenate(halves(matrix), axis=1)


def split(x):
    high = x.astype(BF)
    low = (x - high.astype(F32)).astype(BF)
    return high, low


def packed(x, shift, keep_high):
    high = x.astype(BF).astype(F32)
    return jnp.where(keep_high, high, pltpu.roll(x - high, shift, 0)).astype(BF)


def half_shifted(tile_of, tiles, begin, end):
    left = lax.broadcasted_iota(jnp.int32, (1, LANE), 1) < HALF
    rolled = {t: pltpu.roll(tile_of(t % (tiles + 1)), HALF, 1) for t in range(begin - 1, end)}
    return jnp.concatenate([jnp.where(left, rolled[t - 1], rolled[t]) for t in range(begin, end)], axis=1)


def own_operand(source, edge_keep, begin, end):
    tiles = source.shape[1] // LANE - 1

    def tile_of(t):
        value = source[:, t * LANE : (t + 1) * LANE]
        return value * edge_keep if t == tiles and edge_keep is not None else value

    high, low = split(half_shifted(tile_of, tiles, begin, end))
    return jnp.concatenate([high, low, high], axis=0)


def rim_operand(rims, edge_keep, begin, end):
    tiles = rims[0].shape[1] // LANE - 1

    def tile_of(t):
        value = jnp.concatenate([rim[:, t * LANE : (t + 1) * LANE].astype(F32) for rim in rims], axis=0)
        return value * edge_keep if t == tiles and edge_keep is not None else value

    edges = half_shifted(tile_of, tiles, begin, end).astype(BF)
    return jnp.concatenate([edges, edges], axis=0)


def window(vert, rows, b, tiles):
    if b == tiles:
        return jnp.concatenate([vert[rows, b * LANE : (b + 1) * LANE], vert[rows, 0:LANE]], axis=1)
    return vert[rows, b * LANE : (b + 2) * LANE]


def across(windows, weights):
    high, low = split(jnp.concatenate(windows, axis=0))
    product = jnp.dot(jnp.concatenate([high, low], axis=1), weights, preferred_element_type=F32)
    return product[:, :LANE] + product[:, LANE:]


def horizontal_pass(vert, g_level, lev, start, count, pieces, high_rows, begin, end):
    tiles = vert.shape[1] // LANE - 1
    for k in range(LEVELS):
        rows = pl.ds(start + k * count, count)
        product = across([window(vert, rows, b, tiles) for b in range(begin, end)], g_level[k])
        for b in range(begin, end):
            at = (b - begin) * count
            for first, size in pieces:
                lev[k, pl.ds(b * high_rows + first, size), :] = product[at : at + size]
                at += size


def responses(lev, diff, count, blocks, dog_gain, hess_gain, row_keep, edge_keep, dog, hess):
    tiles = dog.shape[2] // LANE
    lane = lax.broadcasted_iota(jnp.int32, (1, LANE), 1)

    high_rows = count + 8
    for b in range(blocks):
        rows = pl.ds(b * high_rows, high_rows)
        level = [lev[k, rows, :] for k in range(LEVELS)]
        for k in range(LEVELS - 1):
            d = level[k + 1] - level[k]
            if b < tiles:
                dog[k, :, b * LANE : (b + 1) * LANE] = (dog_gain * d[:count]).astype(BF)
            if k in (1, 2):
                d = d * row_keep
                if b == tiles:
                    d = d * edge_keep
                diff[k - 1, rows, :] = d
    if blocks == tiles:
        diff[:, pl.ds(tiles * high_rows, high_rows), :] = jnp.zeros((2, high_rows, LANE), F32)

    def block(b):
        before, after = (b - 1) % (tiles + 1), (b + 1) % (tiles + 1)
        for m in range(2):
            centre = diff[m, pl.ds(b * high_rows, high_rows), :]
            previous = diff[m, pl.ds(before * high_rows, high_rows), :]
            following = diff[m, pl.ds(after * high_rows, high_rows), :]
            right = pltpu.roll(jnp.where(lane == 0, following, centre), LANE - 1, 1)
            left = pltpu.roll(jnp.where(lane == LANE - 1, previous, centre), 1, 1)
            slope = right - left
            dxx = (right + left - 2.0 * centre)[:count]
            twice = 2.0 * centre
            dyy = (
                pltpu.roll(centre, high_rows - 1, 0) + pltpu.roll(centre, 1, 0) - twice
            )[:count]
            dxy = (pltpu.roll(slope, high_rows - 1, 0) - pltpu.roll(slope, 1, 0))[:count] * 0.25
            hess[m, :, b * LANE : (b + 1) * LANE] = (hess_gain * (dxx * dyy - dxy * dxy)).astype(BF)

    for b in range(tiles):
        block(b)

def row_mask(count, before, after):
    index = lax.broadcasted_iota(jnp.int32, (count + 8, 1), 0)
    gone = jnp.logical_or(
        jnp.logical_and(index == count, jnp.logical_not(after)),
        jnp.logical_and(index == count + 7, jnp.logical_not(before)),
    )
    return jnp.where(gone, 0.0, 1.0).astype(F32)


def kernel(
    rows_total, image, a_fine_far, a_rim_far, a_coarse_far, g_level_far, g_base_far,
    dog_fine, hess_fine, cext, crim, a_coarse, g_level,
    ext, rim_out, rim_in, crim_out, vert, lev, diff, base, a_fine, a_rim, g_base,
    load_sem, fsend, frecv, csend, crecv,
):
    tile_rows, tile_cols = image.shape
    tiles = tile_cols // LANE
    strip = tile_rows // 4
    half_cols = tile_cols // 2
    r = lax.axis_index("row")
    c = lax.axis_index("col")
    other = 1 - c
    has_up = r > 0
    has_down = r < rows_total - 1

    load = pltpu.make_async_copy(image, ext.at[pl.ds(0, tile_rows), pl.ds(0, tile_cols)], load_sem.at[0])
    load.start()
    pairs = [
        (a_fine_far, a_fine), (g_level_far, g_level), (g_base_far, g_base), (a_rim_far, a_rim), (a_coarse_far, a_coarse)
    ]
    weights = [
        pltpu.make_async_copy(far, near, load_sem.at[1 + i]) for i, (far, near) in enumerate(pairs)
    ]

    barrier = pltpu.get_barrier_semaphore()

    def greet(row, col):
        pl.semaphore_signal(barrier, inc=1, device_id={"row": row, "col": col}, device_id_type=MESH)

    greet(r, other)

    @pl.when(has_up)
    def _():
        greet(r - 1, c)
        greet(r - 1, other)

    @pl.when(has_down)
    def _():
        greet(r + 1, c)
        greet(r + 1, other)

    load.wait()
    for weight in weights:
        weight.start()

    slot = lax.broadcasted_iota(jnp.int32, (RIM, 1), 0)

    def pack(j):
        part = slice(j * CHUNK * LANE, (j + 1) * CHUNK * LANE)
        rim_out[0, :, part] = packed(ext[0:RIM, part], NEED, slot < NEED)
        rim_out[1, :, part] = packed(ext[tile_rows - RIM : tile_rows, part], SPARE, slot >= SPARE)

    for j in range(tiles // CHUNK):
        pack(j)

    ends = (r == 0).astype(jnp.int32) + (r == rows_total - 1).astype(jnp.int32)
    pl.semaphore_wait(barrier, 5 - 2 * ends)

    def remote(src, dst, send, recv, row, col):
        return pltpu.make_async_remote_copy(
            src_ref=src, dst_ref=dst, send_sem=send, recv_sem=recv,
            device_id={"row": row, "col": col}, device_id_type=MESH,
        )

    edge = pl.ds(pl.multiple_of(other * (tile_cols - LANE), LANE), LANE)
    own = pl.ds(0, tile_cols)
    rim = pl.ds(tile_cols, LANE)
    inner = pl.ds(0, tile_rows)
    first, last, above, below = rim_out.at[0], rim_out.at[1], rim_in.at[0], rim_in.at[1]
    whole = pl.ds(0, RIM)

    chunks = tiles // CHUNK
    span = CHUNK * LANE
    to_down, to_up = [], []
    for j in range(chunks):
        part = pl.ds(j * span, span)
        to_down.append(remote(last.at[whole, part], above.at[whole, part], fsend.at[2 * j], frecv.at[2 * j], r + 1, c))
        to_up.append(
            remote(first.at[whole, part], below.at[whole, part], fsend.at[2 * j + 1], frecv.at[2 * j + 1], r - 1, c)
        )
    n = 2 * chunks
    to_down_corner = remote(last.at[whole, edge], above.at[whole, rim], fsend.at[n], frecv.at[n], r + 1, other)
    to_up_corner = remote(first.at[whole, edge], below.at[whole, rim], fsend.at[n + 1], frecv.at[n + 1], r - 1, other)
    to_side = remote(ext.at[inner, edge], ext.at[inner, rim], fsend.at[n + 2], frecv.at[n + 2], r, other)

    @pl.when(has_down)
    def _():
        to_down_corner.start()
        to_down[0].start()

    @pl.when(has_up)
    def _():
        to_up_corner.start()
        for send in to_up:
            send.start()

    @pl.when(has_down)
    def _():
        for send in to_down[1:]:
            send.start()

    to_side.start()

    wide = tile_cols + LANE

    @pl.when(r == 0)
    def _():
        rim_in[0, :, :] = jnp.zeros((RIM, wide), BF)

    @pl.when(r == rows_total - 1)
    def _():
        rim_in[1, :, :] = jnp.zeros((RIM, wide), BF)

    cext[:, pl.ds(tile_cols, LANE)] = jnp.zeros((2 * strip, LANE), F32)
    crim[:, pl.ds(tile_cols, LANE)] = jnp.zeros((RIM, LANE), BF)

    @pl.when(jnp.logical_or(jnp.logical_and(r == 0, c == 0), jnp.logical_and(r == rows_total - 1, c == 1)))
    def _():
        crim[:, own] = jnp.zeros((RIM, tile_cols), BF)

    for weight in weights:
        weight.wait()
    to_side.wait()

    lane = lax.broadcasted_iota(jnp.int32, (1, LANE), 1)
    keep = jnp.where((lane < HALF) == (c == 0), 1.0, 0.0).astype(F32)
    half_rows = tile_rows // 2
    base_edge = EDGE // 2
    high_rows = tile_rows + RING
    edge_rows = 2 * EDGE + RING
    edge_pieces = [(0, EDGE), (tile_rows - EDGE, EDGE + RING)]
    middle_rows = tile_rows - 2 * EDGE
    middle_at = a_rim.shape[0]

    def base_pass(start, count, pieces, begin, end):
        rows = pl.ds(start, count)
        product = across([vert[rows, 2 * b * LANE : (2 * b + 3) * LANE] for b in range(begin, end)], g_base[...])
        for b in range(begin, end):
            at = (b - begin) * count
            for first_row, size in pieces:
                base[pl.ds(first_row, size), b * LANE : (b + 1) * LANE] = product[at : at + size]
                at += size

    def own_pass(begin, end):
        vert[:, begin * LANE : end * LANE] = jnp.dot(
            a_fine[...], own_operand(ext, keep, begin, end), preferred_element_type=F32
        )

    def rim_pass(begin, end):
        vert[0:middle_at, begin * LANE : end * LANE] += jnp.dot(
            a_rim[...], rim_operand(rim_in_pair, keep, begin, end), preferred_element_type=F32
        )

    rim_in_pair = [above, below]
    ready_at = [CHUNK * (j + 1) + (1 if j == chunks - 1 else 0) for j in range(chunks)]
    base_at = [0] + [(ready - 1) // 2 for ready in ready_at]
    block_at = [0] + [ready - 1 for ready in ready_at[:-1]] + [tiles + 1]
    for j in range(chunks):
        own_pass(CHUNK * j, ready_at[j])
        base_pass(
            middle_at, half_rows - 2 * base_edge, [(base_edge, half_rows - 2 * base_edge)], base_at[j], base_at[j + 1]
        )
        horizontal_pass(
            vert, g_level, lev, middle_at + half_rows - 2 * base_edge, middle_rows,
            [(EDGE, middle_rows)], high_rows, block_at[j], block_at[j + 1],
        )

    @pl.when(has_up)
    def _():
        to_down_corner.wait_recv()

    @pl.when(has_down)
    def _():
        to_up_corner.wait_recv()

    sends, ups, downs = [], [], []
    for j in range(chunks):

        @pl.when(has_up)
        def _():
            to_down[j].wait_recv()

        @pl.when(has_down)
        def _():
            to_up[j].wait_recv()

        rim_pass(CHUNK * j, ready_at[j])
        base_pass(
            0, 2 * base_edge, [(0, base_edge), (half_rows - base_edge, base_edge)], base_at[j], base_at[j + 1]
        )

        columns = (base_at[j + 1] - base_at[j]) * LANE
        near = pl.ds(base_at[j] * LANE, columns)
        mine = pl.ds(pl.multiple_of(c * half_cols + base_at[j] * LANE, LANE), columns)
        crim_out[0, :, near] = packed(base[0:RIM, near], NEED, slot < NEED)
        crim_out[1, :, near] = packed(base[half_rows - RIM : half_rows, near], SPARE, slot >= SPARE)
        up = remote(
            crim_out.at[0, :, near], crim.at[:, mine], csend.at[3 * j], crecv.at[3 * j + c], r - 1, 1
        )
        down = remote(
            crim_out.at[1, :, near], crim.at[:, mine], csend.at[3 * j + 1], crecv.at[3 * j + c], r + 1, 0
        )
        pair = remote(base.at[:, near], cext.at[:, mine], csend.at[3 * j + 2], crecv.at[3 * j + 2], r, other)
        ups.append(up)
        downs.append(down)
        sends.append(pair)

        @pl.when(has_up)
        def _():
            up.start()

        @pl.when(has_down)
        def _():
            down.start()

        pair.start()
        cext[:, mine] = base[:, near]
        horizontal_pass(
            vert, g_level, lev, 2 * base_edge, edge_rows, edge_pieces, high_rows, block_at[j], block_at[j + 1]
        )

    edge_keep = jnp.where(lane == jnp.where(c == 0, 0, LANE - 1), 1.0, 0.0).astype(F32)
    responses(
        lev, diff, tile_rows, tiles + 1, 20.0, 5000.0,
        row_mask(tile_rows, has_up, has_down), edge_keep, dog_fine, hess_fine,
    )

    for send in sends:
        send.wait_recv()

    @pl.when(jnp.logical_or(c == 1, has_up))
    def _():
        @pl.when(jnp.logical_or(c == 0, has_down))
        def _():
            for j in range(chunks):
                for index in range(2):
                    pltpu.make_async_remote_copy(
                        src_ref=ups[j].src_ref, dst_ref=ups[j].dst_ref,
                        send_sem=csend.at[3 * j], recv_sem=crecv.at[3 * j + index],
                        device_id={"row": r, "col": other}, device_id_type=MESH,
                    ).wait_recv()

    @pl.when(has_down)
    def _():
        to_down_corner.wait_send()
        for send in to_down + downs:
            send.wait_send()

    @pl.when(has_up)
    def _():
        to_up_corner.wait_send()
        for send in to_up + ups:
            send.wait_send()

    for send in sends:
        send.wait_send()


def finish(
    rows_total, dog_near, hess_near, cext, crim, a_coarse, g_level,
    dog_fine, hess_fine, dog_coarse, hess_coarse,
    vert, lev, diff, dog, hess, sem,
):
    strip = cext.shape[0] // 2
    tiles = cext.shape[1] // LANE - 1
    r = lax.axis_index("row")
    c = lax.axis_index("col")
    fine = [
        pltpu.make_async_copy(dog_near, dog_fine, sem.at[0]),
        pltpu.make_async_copy(hess_near, hess_fine, sem.at[1]),
    ]
    for copy in fine:
        copy.start()
    for begin in range(0, tiles, CHUNK):
        end = begin + CHUNK + (1 if begin + CHUNK == tiles else 0)
        operand = jnp.concatenate(
            [own_operand(cext, None, begin, end), rim_operand([crim], None, begin, end)], axis=0
        )
        vert[:, begin * LANE : end * LANE] = jnp.dot(a_coarse[c], operand, preferred_element_type=F32)
    horizontal_pass(vert, g_level, lev, 0, strip + RING, [(0, strip + RING)], strip + RING, 0, tiles)
    responses(
        lev, diff, strip, tiles, 80.0, 200000.0,
        row_mask(strip, jnp.logical_or(r > 0, c == 1), jnp.logical_or(r < rows_total - 1, c == 0)),
        None, dog, hess,
    )
    coarse = [
        pltpu.make_async_copy(dog, dog_coarse, sem.at[2]),
        pltpu.make_async_copy(hess, hess_coarse, sem.at[3]),
    ]
    for copy in coarse:
        copy.start()
    for copy in fine + coarse:
        copy.wait()


def solution(mesh):
    rows_total = mesh.shape["row"]

    def local(image):
        tile_rows, tile_cols = image.shape
        strip = tile_rows // 4
        tiles = tile_cols // LANE
        base_edge = EDGE // 2
        half_rows = tile_rows // 2
        numbers = np.arange(half_rows, dtype=np.float64)
        level_rows = ring_rows(tile_rows)

        def fine_matrix(base_rows, rows, inputs):
            matrix = np.concatenate(
                [vertical_matrix(2.0 * base_rows, inputs, SIGMAS[4])]
                + [vertical_matrix(rows, inputs, s) for s in SIGMAS]
            )
            return pad_rows(matrix, 16)

        def edges_of(x, edge, length):
            return np.concatenate([x[:edge], x[length - edge :]])

        fine_in = np.arange(tile_rows, dtype=np.float64)
        edge_out = edges_of(numbers, base_edge, half_rows), edges_of(level_rows, EDGE, tile_rows)
        middle_out = numbers[base_edge : half_rows - base_edge], level_rows[EDGE : tile_rows - EDGE]
        a_fine = own_weights(np.concatenate([fine_matrix(*edge_out, fine_in), fine_matrix(*middle_out, fine_in)]))
        a_rim = rim_weights(fine_matrix(*edge_out, rim_inputs(tile_rows)))
        coarse_out = [strip * c + ring_rows(strip) for c in range(2)]
        coarse_rim = [rim_inputs(2 * strip)[:RIM], rim_inputs(2 * strip)[RIM:]]

        def coarse_matrix(c, inputs):
            return pad_rows(np.concatenate([vertical_matrix(coarse_out[c], inputs, s) for s in SIGMAS]), 16)

        a_coarse = np.stack(
            [
                np.concatenate(
                    [
                        own_weights(coarse_matrix(c, np.arange(2 * strip, dtype=np.float64))),
                        rim_weights(coarse_matrix(c, coarse_rim[c])),
                    ],
                    axis=1,
                )
                for c in range(2)
            ]
        )
        span = np.arange(2 * LANE, dtype=np.float64)[:, None] - HALF
        g_level = np.stack(
            [column_weights(taps_at(s, span - np.arange(LANE)[None, :])) for s in SIGMAS]
        )
        wider = np.arange(3 * LANE, dtype=np.float64)[:, None] - HALF
        g_base = column_weights(taps_at(SIGMAS[4], wider - 2.0 * np.arange(LANE)[None, :]))

        vmem = pl.BlockSpec(memory_space=pltpu.VMEM)
        ring = tile_rows + 8
        wide = tile_cols + LANE
        chunks = tiles // CHUNK
        hbm = pl.BlockSpec(memory_space=pltpu.HBM)
        near = pl.pallas_call(
            functools.partial(kernel, rows_total),
            out_shape=(
                pltpu.VMEM((4, tile_rows, tile_cols), BF),
                pltpu.VMEM((2, tile_rows, tile_cols), BF),
                pltpu.VMEM((2 * strip, wide), F32),
                pltpu.VMEM((RIM, wide), BF),
                pltpu.VMEM(a_coarse.shape, BF),
                pltpu.VMEM(g_level.shape, BF),
            ),
            in_specs=[hbm] * 6,
            out_specs=(vmem,) * 6,
            scratch_shapes=[
                pltpu.VMEM((tile_rows, wide), F32),
                pltpu.VMEM((2, RIM, tile_cols), BF),
                pltpu.VMEM((2, RIM, wide), BF),
                pltpu.VMEM((2, RIM, tile_cols // 2), BF),
                pltpu.VMEM((a_fine.shape[0], wide), F32),
                pltpu.VMEM((LEVELS, (tiles + 1) * ring, LANE), F32),
                pltpu.VMEM((2, (tiles + 1) * ring, LANE), F32),
                pltpu.VMEM((tile_rows // 2, tile_cols // 2), F32),
                pltpu.VMEM(a_fine.shape, BF),
                pltpu.VMEM(a_rim.shape, BF),
                pltpu.VMEM(g_base.shape, BF),
                pltpu.SemaphoreType.DMA((6,)),
                pltpu.SemaphoreType.DMA((2 * chunks + 3,)),
                pltpu.SemaphoreType.DMA((2 * chunks + 3,)),
                pltpu.SemaphoreType.DMA((3 * chunks,)),
                pltpu.SemaphoreType.DMA((3 * chunks,)),
            ],
            compiler_params=pltpu.CompilerParams(
                collective_id=0, has_side_effects=True, vmem_limit_bytes=32000000
            ),
        )(*[pltpu.with_memory_space_constraint(x, pltpu.HBM) for x in (image, a_fine, a_rim, a_coarse, g_level, g_base)])
        coarse_ring = strip + 8
        return pl.pallas_call(
            functools.partial(finish, rows_total),
            out_shape=(
                jax.ShapeDtypeStruct((4, tile_rows, tile_cols), BF),
                jax.ShapeDtypeStruct((2, tile_rows, tile_cols), BF),
                jax.ShapeDtypeStruct((4, strip, tile_cols), BF),
                jax.ShapeDtypeStruct((2, strip, tile_cols), BF),
            ),
            in_specs=[vmem] * 6,
            out_specs=(hbm,) * 4,
            scratch_shapes=[
                pltpu.VMEM((a_coarse.shape[1], wide), F32),
                pltpu.VMEM((LEVELS, tiles * coarse_ring, LANE), F32),
                pltpu.VMEM((2, (tiles + 1) * coarse_ring, LANE), F32),
                pltpu.VMEM((4, strip, tile_cols), BF),
                pltpu.VMEM((2, strip, tile_cols), BF),
                pltpu.SemaphoreType.DMA((4,)),
            ],
            compiler_params=pltpu.CompilerParams(vmem_limit_bytes=32000000),
        )(*near)

    return jax.shard_map(
        local,
        mesh=mesh,
        in_specs=(P(("slab", "row"), "col"),),
        out_specs=(
            P(None, ("slab", "row"), "col"),
            P(None, ("slab", "row"), "col"),
            P(None, ("slab", "row", "col"), None),
            P(None, ("slab", "row", "col"), None),
        ),
        check_vma=False,
    )
```

```python
import functools

import jax
import jax.numpy as jnp
import numpy as np
from jax import lax
from jax.experimental import pallas as pl
from jax.experimental.pallas import tpu as pltpu
from jax.sharding import PartitionSpec as P

SIGMAS = [1.6 * 2.0 ** (k / 4.0) for k in range(5)]
LEVELS = 5
LANE = 128
HALF = LANE // 2
RIM = 16
NEED = 13
SPARE = RIM - NEED
EDGE = 16
RING = 8
CHUNK = 4
MESH = pl.DeviceIdType.MESH
BF = jnp.bfloat16
F32 = jnp.float32


def taps_at(sigma, offset):
    spread = np.arange(25, dtype=np.float64) - 12.0
    total = np.sum(np.exp(-spread * spread / (2.0 * sigma * sigma)))
    weight = np.exp(-(offset**2) / (2.0 * sigma * sigma)) / total
    return np.where(np.abs(offset) <= 12, weight, 0.0)


def halves(matrix):
    high = matrix.astype(BF)
    low = (matrix - high.astype(np.float64)).astype(BF)
    return high, low


def ring_rows(count):
    rows = np.full(count + 8, 10**6, dtype=np.float64)
    rows[: count + 1] = np.arange(count + 1)
    rows[-1] = -1
    return rows


def vertical_matrix(out_rows, in_rows, sigma):
    return taps_at(sigma, in_rows[None, :] - out_rows[:, None])


def pad_rows(matrix, multiple):
    return np.pad(matrix, ((0, -matrix.shape[0] % multiple), (0, 0)))


def column_weights(matrix):
    high, low = halves(matrix)
    pair = np.concatenate([high, low], axis=1)
    return np.concatenate([pair, pair], axis=0)


def rim_inputs(count):
    slot = np.arange(RIM, dtype=np.float64)
    above = np.where(slot >= SPARE, slot - RIM, slot - SPARE)
    below = count + np.where(slot < NEED, slot, slot - NEED)
    return np.concatenate([above, below])


def own_weights(matrix):
    high, low = halves(matrix)
    return np.concatenate([high, high, low], axis=1)


def rim_weights(matrix):
    return np.concatenate(halves(matrix), axis=1)


def split(x):
    high = x.astype(BF)
    low = (x - high.astype(F32)).astype(BF)
    return high, low


def packed(x, shift, keep_high):
    high = x.astype(BF).astype(F32)
    return jnp.where(keep_high, high, pltpu.roll(x - high, shift, 0)).astype(BF)


def half_shifted(tile_of, tiles, begin, end):
    left = lax.broadcasted_iota(jnp.int32, (1, LANE), 1) < HALF
    rolled = {t: pltpu.roll(tile_of(t % (tiles + 1)), HALF, 1) for t in range(begin - 1, end)}
    return jnp.concatenate([jnp.where(left, rolled[t - 1], rolled[t]) for t in range(begin, end)], axis=1)


def own_operand(source, edge_keep, begin, end):
    tiles = source.shape[1] // LANE - 1

    def tile_of(t):
        value = source[:, t * LANE : (t + 1) * LANE]
        return value * edge_keep if t == tiles and edge_keep is not None else value

    high, low = split(half_shifted(tile_of, tiles, begin, end))
    return jnp.concatenate([high, low, high], axis=0)


def rim_operand(rims, edge_keep, begin, end):
    tiles = rims[0].shape[1] // LANE - 1

    def tile_of(t):
        value = jnp.concatenate([rim[:, t * LANE : (t + 1) * LANE].astype(F32) for rim in rims], axis=0)
        return value * edge_keep if t == tiles and edge_keep is not None else value

    edges = half_shifted(tile_of, tiles, begin, end).astype(BF)
    return jnp.concatenate([edges, edges], axis=0)


def window(vert, rows, b, tiles):
    if b == tiles:
        return jnp.concatenate([vert[rows, b * LANE : (b + 1) * LANE], vert[rows, 0:LANE]], axis=1)
    return vert[rows, b * LANE : (b + 2) * LANE]


def across(windows, weights):
    high, low = split(jnp.concatenate(windows, axis=0))
    product = jnp.dot(jnp.concatenate([high, low], axis=1), weights, preferred_element_type=F32)
    return product[:, :LANE] + product[:, LANE:]


def horizontal_pass(vert, g_level, lev, start, count, pieces, high_rows, begin, end):
    tiles = vert.shape[1] // LANE - 1
    for k in range(LEVELS):
        rows = pl.ds(start + k * count, count)
        product = across([window(vert, rows, b, tiles) for b in range(begin, end)], g_level[k])
        for b in range(begin, end):
            at = (b - begin) * count
            for first, size in pieces:
                lev[k, pl.ds(b * high_rows + first, size), :] = product[at : at + size]
                at += size


def responses(lev, diff, count, blocks, dog_gain, hess_gain, row_keep, edge_keep, dog, hess):
    tiles = dog.shape[2] // LANE
    lane = lax.broadcasted_iota(jnp.int32, (1, LANE), 1)

    high_rows = count + 8
    for b in range(blocks):
        rows = pl.ds(b * high_rows, high_rows)
        level = [lev[k, rows, :] for k in range(LEVELS)]
        for k in range(LEVELS - 1):
            d = level[k + 1] - level[k]
            if b < tiles:
                dog[k, :, b * LANE : (b + 1) * LANE] = (dog_gain * d[:count]).astype(BF)
            if k in (1, 2):
                d = d * row_keep
                if b == tiles:
                    d = d * edge_keep
                diff[k - 1, rows, :] = d
    if blocks == tiles:
        diff[:, pl.ds(tiles * high_rows, high_rows), :] = jnp.zeros((2, high_rows, LANE), F32)

    def block(b):
        before, after = (b - 1) % (tiles + 1), (b + 1) % (tiles + 1)
        for m in range(2):
            centre = diff[m, pl.ds(b * high_rows, high_rows), :]
            previous = diff[m, pl.ds(before * high_rows, high_rows), :]
            following = diff[m, pl.ds(after * high_rows, high_rows), :]
            right = pltpu.roll(jnp.where(lane == 0, following, centre), LANE - 1, 1)
            left = pltpu.roll(jnp.where(lane == LANE - 1, previous, centre), 1, 1)
            slope = right - left
            dxx = (right + left - 2.0 * centre)[:count]
            twice = 2.0 * centre
            dyy = (
                pltpu.roll(centre, high_rows - 1, 0) + pltpu.roll(centre, 1, 0) - twice
            )[:count]
            dxy = (pltpu.roll(slope, high_rows - 1, 0) - pltpu.roll(slope, 1, 0))[:count] * 0.25
            hess[m, :, b * LANE : (b + 1) * LANE] = (hess_gain * (dxx * dyy - dxy * dxy)).astype(BF)

    for b in range(tiles):
        block(b)

def row_mask(count, before, after):
    index = lax.broadcasted_iota(jnp.int32, (count + 8, 1), 0)
    gone = jnp.logical_or(
        jnp.logical_and(index == count, jnp.logical_not(after)),
        jnp.logical_and(index == count + 7, jnp.logical_not(before)),
    )
    return jnp.where(gone, 0.0, 1.0).astype(F32)


def kernel(
    rows_total, image, a_fine_far, a_rim_far, a_coarse_far, g_level_far, g_base_far,
    dog_fine, hess_fine, cext, crim, a_coarse, g_level,
    ext, rim_out, rim_in, crim_out, vert, lev, diff, base, a_fine, a_rim, g_base,
    load_sem, fsend, frecv, csend, crecv,
):
    tile_rows, tile_cols = image.shape
    tiles = tile_cols // LANE
    strip = tile_rows // 4
    half_cols = tile_cols // 2
    r = lax.axis_index("row")
    c = lax.axis_index("col")
    other = 1 - c
    has_up = r > 0
    has_down = r < rows_total - 1

    load = pltpu.make_async_copy(image, ext.at[pl.ds(0, tile_rows), pl.ds(0, tile_cols)], load_sem.at[0])
    load.start()
    pairs = [
        (a_fine_far, a_fine), (g_level_far, g_level), (g_base_far, g_base), (a_rim_far, a_rim), (a_coarse_far, a_coarse)
    ]
    weights = [
        pltpu.make_async_copy(far, near, load_sem.at[1 + i]) for i, (far, near) in enumerate(pairs)
    ]

    barrier = pltpu.get_barrier_semaphore()

    def greet(row, col):
        pl.semaphore_signal(barrier, inc=1, device_id={"row": row, "col": col}, device_id_type=MESH)

    greet(r, other)

    @pl.when(has_up)
    def _():
        greet(r - 1, c)
        greet(r - 1, other)

    @pl.when(has_down)
    def _():
        greet(r + 1, c)
        greet(r + 1, other)

    load.wait()
    for weight in weights:
        weight.start()

    slot = lax.broadcasted_iota(jnp.int32, (RIM, 1), 0)

    def pack(j):
        part = slice(j * CHUNK * LANE, (j + 1) * CHUNK * LANE)
        rim_out[0, :, part] = packed(ext[0:RIM, part], NEED, slot < NEED)
        rim_out[1, :, part] = packed(ext[tile_rows - RIM : tile_rows, part], SPARE, slot >= SPARE)

    for j in range(tiles // CHUNK):
        pack(j)

    ends = (r == 0).astype(jnp.int32) + (r == rows_total - 1).astype(jnp.int32)
    pl.semaphore_wait(barrier, 5 - 2 * ends)

    def remote(src, dst, send, recv, row, col):
        return pltpu.make_async_remote_copy(
            src_ref=src, dst_ref=dst, send_sem=send, recv_sem=recv,
            device_id={"row": row, "col": col}, device_id_type=MESH,
        )

    edge = pl.ds(pl.multiple_of(other * (tile_cols - LANE), LANE), LANE)
    own = pl.ds(0, tile_cols)
    rim = pl.ds(tile_cols, LANE)
    inner = pl.ds(0, tile_rows)
    first, last, above, below = rim_out.at[0], rim_out.at[1], rim_in.at[0], rim_in.at[1]
    whole = pl.ds(0, RIM)

    chunks = tiles // CHUNK
    ready_at = [CHUNK * (j + 1) + 1 for j in range(chunks)]
    arrive_at = [0] + ready_at[:-1] + [tiles]
    to_down, to_up = [], []
    for j in range(chunks):
        part = pl.ds(arrive_at[j] * LANE, (arrive_at[j + 1] - arrive_at[j]) * LANE)
        to_down.append(remote(last.at[whole, part], above.at[whole, part], fsend.at[2 * j], frecv.at[2 * j], r + 1, c))
        to_up.append(
            remote(first.at[whole, part], below.at[whole, part], fsend.at[2 * j + 1], frecv.at[2 * j + 1], r - 1, c)
        )
    n = 2 * chunks
    to_down_corner = remote(last.at[whole, edge], above.at[whole, rim], fsend.at[n], frecv.at[n], r + 1, other)
    to_up_corner = remote(first.at[whole, edge], below.at[whole, rim], fsend.at[n + 1], frecv.at[n + 1], r - 1, other)
    to_side = remote(ext.at[inner, edge], ext.at[inner, rim], fsend.at[n + 2], frecv.at[n + 2], r, other)

    @pl.when(has_down)
    def _():
        to_down_corner.start()

    @pl.when(has_up)
    def _():
        to_up_corner.start()

    def start_if(condition, send):
        @pl.when(condition)
        def _():
            send.start()

    for j in range(chunks):
        start_if(has_down, to_down[j])
        start_if(has_up, to_up[j])

    to_side.start()

    wide = tile_cols + LANE

    @pl.when(r == 0)
    def _():
        rim_in[0, :, :] = jnp.zeros((RIM, wide), BF)

    @pl.when(r == rows_total - 1)
    def _():
        rim_in[1, :, :] = jnp.zeros((RIM, wide), BF)

    cext[:, pl.ds(tile_cols, LANE)] = jnp.zeros((2 * strip, LANE), F32)
    crim[:, pl.ds(tile_cols, LANE)] = jnp.zeros((RIM, LANE), BF)

    @pl.when(jnp.logical_or(jnp.logical_and(r == 0, c == 0), jnp.logical_and(r == rows_total - 1, c == 1)))
    def _():
        crim[:, own] = jnp.zeros((RIM, tile_cols), BF)

    for weight in weights:
        weight.wait()
    to_side.wait()

    lane = lax.broadcasted_iota(jnp.int32, (1, LANE), 1)
    keep = jnp.where((lane < HALF) == (c == 0), 1.0, 0.0).astype(F32)
    half_rows = tile_rows // 2
    base_edge = EDGE // 2
    high_rows = tile_rows + RING
    edge_rows = 2 * EDGE + RING
    edge_pieces = [(0, EDGE), (tile_rows - EDGE, EDGE + RING)]
    middle_rows = tile_rows - 2 * EDGE
    middle_at = a_rim.shape[0]

    def base_pass(start, count, pieces, begin, end):
        rows = pl.ds(start, count)
        product = across([vert[rows, 2 * b * LANE : (2 * b + 3) * LANE] for b in range(begin, end)], g_base[...])
        for b in range(begin, end):
            at = (b - begin) * count
            for first_row, size in pieces:
                base[pl.ds(first_row, size), b * LANE : (b + 1) * LANE] = product[at : at + size]
                at += size

    def own_pass(begin, end):
        vert[:, begin * LANE : end * LANE] = jnp.dot(
            a_fine[...], own_operand(ext, keep, begin, end), preferred_element_type=F32
        )

    base_rows = 2 * base_edge

    def rim_pass(rows, begin, end):
        vert[rows, begin * LANE : end * LANE] += jnp.dot(
            a_rim[rows, :], rim_operand(rim_in_pair, keep, begin, end), preferred_element_type=F32
        )

    rim_in_pair = [above, below]
    start_at = [0] + ready_at[:-1]
    base_at = [0] + [(ready - 1) // 2 for ready in ready_at]
    block_at = [0] + [ready - 1 for ready in ready_at[:-1]] + [tiles + 1]
    for j in range(chunks):
        own_pass(start_at[j], ready_at[j])
        base_pass(
            middle_at, half_rows - 2 * base_edge, [(base_edge, half_rows - 2 * base_edge)], base_at[j], base_at[j + 1]
        )
        horizontal_pass(
            vert, g_level, lev, middle_at + half_rows - 2 * base_edge, middle_rows,
            [(EDGE, middle_rows)], high_rows, block_at[j], block_at[j + 1],
        )

    @pl.when(has_up)
    def _():
        to_down_corner.wait_recv()

    @pl.when(has_down)
    def _():
        to_up_corner.wait_recv()

    sends, ups, downs = [], [], []
    for j in range(chunks):

        @pl.when(has_up)
        def _():
            to_down[j].wait_recv()

        @pl.when(has_down)
        def _():
            to_up[j].wait_recv()

        rim_pass(slice(0, base_rows), start_at[j], ready_at[j])
        base_pass(
            0, base_rows, [(0, base_edge), (half_rows - base_edge, base_edge)], base_at[j], base_at[j + 1]
        )

        columns = (base_at[j + 1] - base_at[j]) * LANE
        near = pl.ds(base_at[j] * LANE, columns)
        mine = pl.ds(pl.multiple_of(c * half_cols + base_at[j] * LANE, LANE), columns)
        crim_out[0, :, near] = packed(base[0:RIM, near], NEED, slot < NEED)
        crim_out[1, :, near] = packed(base[half_rows - RIM : half_rows, near], SPARE, slot >= SPARE)
        up = remote(
            crim_out.at[0, :, near], crim.at[:, mine], csend.at[3 * j], crecv.at[3 * j + c], r - 1, 1
        )
        down = remote(
            crim_out.at[1, :, near], crim.at[:, mine], csend.at[3 * j + 1], crecv.at[3 * j + c], r + 1, 0
        )
        pair = remote(base.at[:, near], cext.at[:, mine], csend.at[3 * j + 2], crecv.at[3 * j + 2], r, other)
        ups.append(up)
        downs.append(down)
        sends.append(pair)

        @pl.when(has_up)
        def _():
            up.start()

        @pl.when(has_down)
        def _():
            down.start()

        pair.start()
        cext[:, mine] = base[:, near]

    for j in range(chunks):
        rim_pass(slice(base_rows, middle_at), start_at[j], ready_at[j])

    for j in range(chunks):
        horizontal_pass(
            vert, g_level, lev, base_rows, edge_rows, edge_pieces, high_rows, block_at[j], block_at[j + 1]
        )

    edge_keep = jnp.where(lane == jnp.where(c == 0, 0, LANE - 1), 1.0, 0.0).astype(F32)
    responses(
        lev, diff, tile_rows, tiles + 1, 20.0, 5000.0,
        row_mask(tile_rows, has_up, has_down), edge_keep, dog_fine, hess_fine,
    )

    for send in sends:
        send.wait_recv()

    @pl.when(jnp.logical_or(c == 1, has_up))
    def _():
        @pl.when(jnp.logical_or(c == 0, has_down))
        def _():
            for j in range(chunks):
                for index in range(2):
                    pltpu.make_async_remote_copy(
                        src_ref=ups[j].src_ref, dst_ref=ups[j].dst_ref,
                        send_sem=csend.at[3 * j], recv_sem=crecv.at[3 * j + index],
                        device_id={"row": r, "col": other}, device_id_type=MESH,
                    ).wait_recv()

    @pl.when(has_down)
    def _():
        to_down_corner.wait_send()
        for send in to_down + downs:
            send.wait_send()

    @pl.when(has_up)
    def _():
        to_up_corner.wait_send()
        for send in to_up + ups:
            send.wait_send()

    for send in sends:
        send.wait_send()


def finish(
    rows_total, dog_near, hess_near, cext, crim, a_coarse, g_level,
    dog_fine, hess_fine, dog_coarse, hess_coarse,
    vert, lev, diff, dog, hess, sem,
):
    strip = cext.shape[0] // 2
    tiles = cext.shape[1] // LANE - 1
    r = lax.axis_index("row")
    c = lax.axis_index("col")
    fine = [
        pltpu.make_async_copy(dog_near, dog_fine, sem.at[0]),
        pltpu.make_async_copy(hess_near, hess_fine, sem.at[1]),
    ]
    for copy in fine:
        copy.start()
    for begin in range(0, tiles, CHUNK):
        end = begin + CHUNK + (1 if begin + CHUNK == tiles else 0)
        operand = jnp.concatenate(
            [own_operand(cext, None, begin, end), rim_operand([crim], None, begin, end)], axis=0
        )
        vert[:, begin * LANE : end * LANE] = jnp.dot(a_coarse[c], operand, preferred_element_type=F32)
    horizontal_pass(vert, g_level, lev, 0, strip + RING, [(0, strip + RING)], strip + RING, 0, tiles)
    responses(
        lev, diff, strip, tiles, 80.0, 200000.0,
        row_mask(strip, jnp.logical_or(r > 0, c == 1), jnp.logical_or(r < rows_total - 1, c == 0)),
        None, dog, hess,
    )
    coarse = [
        pltpu.make_async_copy(dog, dog_coarse, sem.at[2]),
        pltpu.make_async_copy(hess, hess_coarse, sem.at[3]),
    ]
    for copy in coarse:
        copy.start()
    for copy in fine + coarse:
        copy.wait()


def solution(mesh):
    rows_total = mesh.shape["row"]

    def local(image):
        tile_rows, tile_cols = image.shape
        strip = tile_rows // 4
        tiles = tile_cols // LANE
        base_edge = EDGE // 2
        half_rows = tile_rows // 2
        numbers = np.arange(half_rows, dtype=np.float64)
        level_rows = ring_rows(tile_rows)

        def fine_matrix(base_rows, rows, inputs):
            matrix = np.concatenate(
                [vertical_matrix(2.0 * base_rows, inputs, SIGMAS[4])]
                + [vertical_matrix(rows, inputs, s) for s in SIGMAS]
            )
            return pad_rows(matrix, 16)

        def edges_of(x, edge, length):
            return np.concatenate([x[:edge], x[length - edge :]])

        fine_in = np.arange(tile_rows, dtype=np.float64)
        edge_out = edges_of(numbers, base_edge, half_rows), edges_of(level_rows, EDGE, tile_rows)
        middle_out = numbers[base_edge : half_rows - base_edge], level_rows[EDGE : tile_rows - EDGE]
        a_fine = own_weights(np.concatenate([fine_matrix(*edge_out, fine_in), fine_matrix(*middle_out, fine_in)]))
        a_rim = rim_weights(fine_matrix(*edge_out, rim_inputs(tile_rows)))
        coarse_out = [strip * c + ring_rows(strip) for c in range(2)]
        coarse_rim = [rim_inputs(2 * strip)[:RIM], rim_inputs(2 * strip)[RIM:]]

        def coarse_matrix(c, inputs):
            return pad_rows(np.concatenate([vertical_matrix(coarse_out[c], inputs, s) for s in SIGMAS]), 16)

        a_coarse = np.stack(
            [
                np.concatenate(
                    [
                        own_weights(coarse_matrix(c, np.arange(2 * strip, dtype=np.float64))),
                        rim_weights(coarse_matrix(c, coarse_rim[c])),
                    ],
                    axis=1,
                )
                for c in range(2)
            ]
        )
        span = np.arange(2 * LANE, dtype=np.float64)[:, None] - HALF
        g_level = np.stack(
            [column_weights(taps_at(s, span - np.arange(LANE)[None, :])) for s in SIGMAS]
        )
        wider = np.arange(3 * LANE, dtype=np.float64)[:, None] - HALF
        g_base = column_weights(taps_at(SIGMAS[4], wider - 2.0 * np.arange(LANE)[None, :]))

        vmem = pl.BlockSpec(memory_space=pltpu.VMEM)
        ring = tile_rows + 8
        wide = tile_cols + LANE
        chunks = tiles // CHUNK
        hbm = pl.BlockSpec(memory_space=pltpu.HBM)
        near = pl.pallas_call(
            functools.partial(kernel, rows_total),
            out_shape=(
                pltpu.VMEM((4, tile_rows, tile_cols), BF),
                pltpu.VMEM((2, tile_rows, tile_cols), BF),
                pltpu.VMEM((2 * strip, wide), F32),
                pltpu.VMEM((RIM, wide), BF),
                pltpu.VMEM(a_coarse.shape, BF),
                pltpu.VMEM(g_level.shape, BF),
            ),
            in_specs=[hbm] * 6,
            out_specs=(vmem,) * 6,
            scratch_shapes=[
                pltpu.VMEM((tile_rows, wide), F32),
                pltpu.VMEM((2, RIM, tile_cols), BF),
                pltpu.VMEM((2, RIM, wide), BF),
                pltpu.VMEM((2, RIM, tile_cols // 2), BF),
                pltpu.VMEM((a_fine.shape[0], wide), F32),
                pltpu.VMEM((LEVELS, (tiles + 1) * ring, LANE), F32),
                pltpu.VMEM((2, (tiles + 1) * ring, LANE), F32),
                pltpu.VMEM((tile_rows // 2, tile_cols // 2), F32),
                pltpu.VMEM(a_fine.shape, BF),
                pltpu.VMEM(a_rim.shape, BF),
                pltpu.VMEM(g_base.shape, BF),
                pltpu.SemaphoreType.DMA((6,)),
                pltpu.SemaphoreType.DMA((2 * chunks + 3,)),
                pltpu.SemaphoreType.DMA((2 * chunks + 3,)),
                pltpu.SemaphoreType.DMA((3 * chunks,)),
                pltpu.SemaphoreType.DMA((3 * chunks,)),
            ],
            compiler_params=pltpu.CompilerParams(
                collective_id=0, has_side_effects=True, vmem_limit_bytes=32000000
            ),
        )(*[pltpu.with_memory_space_constraint(x, pltpu.HBM) for x in (image, a_fine, a_rim, a_coarse, g_level, g_base)])
        coarse_ring = strip + 8
        return pl.pallas_call(
            functools.partial(finish, rows_total),
            out_shape=(
                jax.ShapeDtypeStruct((4, tile_rows, tile_cols), BF),
                jax.ShapeDtypeStruct((2, tile_rows, tile_cols), BF),
                jax.ShapeDtypeStruct((4, strip, tile_cols), BF),
                jax.ShapeDtypeStruct((2, strip, tile_cols), BF),
            ),
            in_specs=[vmem] * 6,
            out_specs=(hbm,) * 4,
            scratch_shapes=[
                pltpu.VMEM((a_coarse.shape[1], wide), F32),
                pltpu.VMEM((LEVELS, tiles * coarse_ring, LANE), F32),
                pltpu.VMEM((2, (tiles + 1) * coarse_ring, LANE), F32),
                pltpu.VMEM((4, strip, tile_cols), BF),
                pltpu.VMEM((2, strip, tile_cols), BF),
                pltpu.SemaphoreType.DMA((4,)),
            ],
            compiler_params=pltpu.CompilerParams(vmem_limit_bytes=32000000),
        )(*near)

    return jax.shard_map(
        local,
        mesh=mesh,
        in_specs=(P(("slab", "row"), "col"),),
        out_specs=(
            P(None, ("slab", "row"), "col"),
            P(None, ("slab", "row"), "col"),
            P(None, ("slab", "row", "col"), None),
            P(None, ("slab", "row", "col"), None),
        ),
        check_vma=False,
    )
```

```python
import functools

import jax
import jax.numpy as jnp
import numpy as np
from jax import lax
from jax.experimental import pallas as pl
from jax.experimental.pallas import tpu as pltpu
from jax.sharding import PartitionSpec as P

SIGMAS = [1.6 * 2.0 ** (k / 4.0) for k in range(5)]
LEVELS = 5
LANE = 128
HALF = LANE // 2
RIM = 16
NEED = 13
SPARE = RIM - NEED
EDGE = 16
RING = 8
CHUNK = 8
MESH = pl.DeviceIdType.MESH
BF = jnp.bfloat16
F32 = jnp.float32


def taps_at(sigma, offset):
    spread = np.arange(25, dtype=np.float64) - 12.0
    total = np.sum(np.exp(-spread * spread / (2.0 * sigma * sigma)))
    weight = np.exp(-(offset**2) / (2.0 * sigma * sigma)) / total
    return np.where(np.abs(offset) <= 12, weight, 0.0)


def halves(matrix):
    high = matrix.astype(BF)
    low = (matrix - high.astype(np.float64)).astype(BF)
    return high, low


def ring_rows(count):
    rows = np.full(count + 8, 10**6, dtype=np.float64)
    rows[: count + 1] = np.arange(count + 1)
    rows[-1] = -1
    return rows


def vertical_matrix(out_rows, in_rows, sigma):
    return taps_at(sigma, in_rows[None, :] - out_rows[:, None])


def pad_rows(matrix, multiple):
    return np.pad(matrix, ((0, -matrix.shape[0] % multiple), (0, 0)))


def column_weights(matrix):
    high, low = halves(matrix)
    pair = np.concatenate([high, low], axis=1)
    return np.concatenate([pair, pair], axis=0)


def rim_inputs(count):
    slot = np.arange(RIM, dtype=np.float64)
    above = np.where(slot >= SPARE, slot - RIM, slot - SPARE)
    below = count + np.where(slot < NEED, slot, slot - NEED)
    return np.concatenate([above, below])


def own_weights(matrix):
    high, low = halves(matrix)
    return np.concatenate([high, high, low], axis=1)


def rim_weights(matrix):
    return np.concatenate(halves(matrix), axis=1)


def split(x):
    high = x.astype(BF)
    low = (x - high.astype(F32)).astype(BF)
    return high, low


def packed(x, shift, keep_high):
    high = x.astype(BF).astype(F32)
    return jnp.where(keep_high, high, pltpu.roll(x - high, shift, 0)).astype(BF)


def half_shifted(tile_of, tiles, begin, end):
    left = lax.broadcasted_iota(jnp.int32, (1, LANE), 1) < HALF
    rolled = {t: pltpu.roll(tile_of(t % (tiles + 1)), HALF, 1) for t in range(begin - 1, end)}
    return jnp.concatenate([jnp.where(left, rolled[t - 1], rolled[t]) for t in range(begin, end)], axis=1)


def own_operand(source, edge_keep, begin, end):
    tiles = source.shape[1] // LANE - 1

    def tile_of(t):
        value = source[:, t * LANE : (t + 1) * LANE]
        return value * edge_keep if t == tiles and edge_keep is not None else value

    high, low = split(half_shifted(tile_of, tiles, begin, end))
    return jnp.concatenate([high, low, high], axis=0)


def rim_operand(rims, edge_keep, begin, end):
    tiles = rims[0].shape[1] // LANE - 1

    def tile_of(t):
        value = jnp.concatenate([rim[:, t * LANE : (t + 1) * LANE].astype(F32) for rim in rims], axis=0)
        return value * edge_keep if t == tiles and edge_keep is not None else value

    edges = half_shifted(tile_of, tiles, begin, end).astype(BF)
    return jnp.concatenate([edges, edges], axis=0)


def window(vert, rows, b, tiles):
    if b == tiles:
        return jnp.concatenate([vert[rows, b * LANE : (b + 1) * LANE], vert[rows, 0:LANE]], axis=1)
    return vert[rows, b * LANE : (b + 2) * LANE]


def across(windows, weights):
    high, low = split(jnp.concatenate(windows, axis=0))
    product = jnp.dot(jnp.concatenate([high, low], axis=1), weights, preferred_element_type=F32)
    return product[:, :LANE] + product[:, LANE:]


def horizontal_pass(vert, g_level, lev, start, count, pieces, high_rows, begin, end):
    tiles = vert.shape[1] // LANE - 1
    for k in range(LEVELS):
        rows = pl.ds(start + k * count, count)
        product = across([window(vert, rows, b, tiles) for b in range(begin, end)], g_level[k])
        for b in range(begin, end):
            at = (b - begin) * count
            for first, size in pieces:
                lev[k, pl.ds(b * high_rows + first, size), :] = product[at : at + size]
                at += size


def responses(lev, diff, count, blocks, dog_gain, hess_gain, row_keep, edge_keep, dog, hess):
    tiles = dog.shape[2] // LANE
    lane = lax.broadcasted_iota(jnp.int32, (1, LANE), 1)

    high_rows = count + 8
    for b in range(blocks):
        rows = pl.ds(b * high_rows, high_rows)
        level = [lev[k, rows, :] for k in range(LEVELS)]
        for k in range(LEVELS - 1):
            d = level[k + 1] - level[k]
            if b < tiles:
                dog[k, :, b * LANE : (b + 1) * LANE] = (dog_gain * d[:count]).astype(BF)
            if k in (1, 2):
                d = d * row_keep
                if b == tiles:
                    d = d * edge_keep
                diff[k - 1, rows, :] = d
    if blocks == tiles:
        diff[:, pl.ds(tiles * high_rows, high_rows), :] = jnp.zeros((2, high_rows, LANE), F32)

    def block(b):
        before, after = (b - 1) % (tiles + 1), (b + 1) % (tiles + 1)
        for m in range(2):
            centre = diff[m, pl.ds(b * high_rows, high_rows), :]
            previous = diff[m, pl.ds(before * high_rows, high_rows), :]
            following = diff[m, pl.ds(after * high_rows, high_rows), :]
            right = pltpu.roll(jnp.where(lane == 0, following, centre), LANE - 1, 1)
            left = pltpu.roll(jnp.where(lane == LANE - 1, previous, centre), 1, 1)
            slope = right - left
            dxx = (right + left - 2.0 * centre)[:count]
            twice = 2.0 * centre
            dyy = (
                pltpu.roll(centre, high_rows - 1, 0) + pltpu.roll(centre, 1, 0) - twice
            )[:count]
            dxy = (pltpu.roll(slope, high_rows - 1, 0) - pltpu.roll(slope, 1, 0))[:count] * 0.25
            hess[m, :, b * LANE : (b + 1) * LANE] = (hess_gain * (dxx * dyy - dxy * dxy)).astype(BF)

    for b in range(tiles):
        block(b)

def row_mask(count, before, after):
    index = lax.broadcasted_iota(jnp.int32, (count + 8, 1), 0)
    gone = jnp.logical_or(
        jnp.logical_and(index == count, jnp.logical_not(after)),
        jnp.logical_and(index == count + 7, jnp.logical_not(before)),
    )
    return jnp.where(gone, 0.0, 1.0).astype(F32)


def kernel(
    rows_total, image, a_fine_far, a_rim_far, a_coarse_far, g_level_far, g_base_far,
    dog_fine, hess_fine, cext, crim, a_coarse, g_level,
    ext, rim_out, rim_in, crim_out, vert, lev, diff, base, a_fine, a_rim, g_base,
    load_sem, fsend, frecv, csend, crecv,
):
    tile_rows, tile_cols = image.shape
    tiles = tile_cols // LANE
    strip = tile_rows // 4
    half_cols = tile_cols // 2
    r = lax.axis_index("row")
    c = lax.axis_index("col")
    other = 1 - c
    has_up = r > 0
    has_down = r < rows_total - 1

    load = pltpu.make_async_copy(image, ext.at[pl.ds(0, tile_rows), pl.ds(0, tile_cols)], load_sem.at[0])
    load.start()
    pairs = [
        (a_fine_far, a_fine), (g_level_far, g_level), (g_base_far, g_base), (a_rim_far, a_rim), (a_coarse_far, a_coarse)
    ]
    weights = [
        pltpu.make_async_copy(far, near, load_sem.at[1 + i]) for i, (far, near) in enumerate(pairs)
    ]

    barrier = pltpu.get_barrier_semaphore()

    def greet(row, col):
        pl.semaphore_signal(barrier, inc=1, device_id={"row": row, "col": col}, device_id_type=MESH)

    greet(r, other)

    @pl.when(has_up)
    def _():
        greet(r - 1, c)
        greet(r - 1, other)

    @pl.when(has_down)
    def _():
        greet(r + 1, c)
        greet(r + 1, other)

    load.wait()
    for weight in weights:
        weight.start()

    slot = lax.broadcasted_iota(jnp.int32, (RIM, 1), 0)

    def pack(j):
        part = slice(j * CHUNK * LANE, (j + 1) * CHUNK * LANE)
        rim_out[0, :, part] = packed(ext[0:RIM, part], NEED, slot < NEED)
        rim_out[1, :, part] = packed(ext[tile_rows - RIM : tile_rows, part], SPARE, slot >= SPARE)

    for j in range(tiles // CHUNK):
        pack(j)

    ends = (r == 0).astype(jnp.int32) + (r == rows_total - 1).astype(jnp.int32)
    pl.semaphore_wait(barrier, 5 - 2 * ends)

    def remote(src, dst, send, recv, row, col):
        return pltpu.make_async_remote_copy(
            src_ref=src, dst_ref=dst, send_sem=send, recv_sem=recv,
            device_id={"row": row, "col": col}, device_id_type=MESH,
        )

    edge = pl.ds(pl.multiple_of(other * (tile_cols - LANE), LANE), LANE)
    own = pl.ds(0, tile_cols)
    rim = pl.ds(tile_cols, LANE)
    inner = pl.ds(0, tile_rows)
    first, last, above, below = rim_out.at[0], rim_out.at[1], rim_in.at[0], rim_in.at[1]
    whole = pl.ds(0, RIM)

    chunks = tiles // CHUNK
    ready_at = [CHUNK * (j + 1) + 1 for j in range(chunks)]
    arrive_at = [0] + ready_at[:-1] + [tiles]
    to_down, to_up = [], []
    for j in range(chunks):
        part = pl.ds(arrive_at[j] * LANE, (arrive_at[j + 1] - arrive_at[j]) * LANE)
        to_down.append(remote(last.at[whole, part], above.at[whole, part], fsend.at[2 * j], frecv.at[2 * j], r + 1, c))
        to_up.append(
            remote(first.at[whole, part], below.at[whole, part], fsend.at[2 * j + 1], frecv.at[2 * j + 1], r - 1, c)
        )
    n = 2 * chunks
    to_down_corner = remote(last.at[whole, edge], above.at[whole, rim], fsend.at[n], frecv.at[n], r + 1, other)
    to_up_corner = remote(first.at[whole, edge], below.at[whole, rim], fsend.at[n + 1], frecv.at[n + 1], r - 1, other)
    to_side = remote(ext.at[inner, edge], ext.at[inner, rim], fsend.at[n + 2], frecv.at[n + 2], r, other)

    @pl.when(has_down)
    def _():
        to_down_corner.start()

    @pl.when(has_up)
    def _():
        to_up_corner.start()

    def start_if(condition, send):
        @pl.when(condition)
        def _():
            send.start()

    for j in range(chunks):
        start_if(has_down, to_down[j])
        start_if(has_up, to_up[j])

    to_side.start()

    wide = tile_cols + LANE

    @pl.when(r == 0)
    def _():
        rim_in[0, :, :] = jnp.zeros((RIM, wide), BF)

    @pl.when(r == rows_total - 1)
    def _():
        rim_in[1, :, :] = jnp.zeros((RIM, wide), BF)

    cext[:, pl.ds(tile_cols, LANE)] = jnp.zeros((2 * strip, LANE), F32)
    crim[:, pl.ds(tile_cols, LANE)] = jnp.zeros((RIM, LANE), BF)

    @pl.when(jnp.logical_or(jnp.logical_and(r == 0, c == 0), jnp.logical_and(r == rows_total - 1, c == 1)))
    def _():
        crim[:, own] = jnp.zeros((RIM, tile_cols), BF)

    for weight in weights:
        weight.wait()
    to_side.wait()

    lane = lax.broadcasted_iota(jnp.int32, (1, LANE), 1)
    keep = jnp.where((lane < HALF) == (c == 0), 1.0, 0.0).astype(F32)
    half_rows = tile_rows // 2
    base_edge = EDGE // 2
    high_rows = tile_rows + RING
    edge_rows = 2 * EDGE + RING
    edge_pieces = [(0, EDGE), (tile_rows - EDGE, EDGE + RING)]
    middle_rows = tile_rows - 2 * EDGE
    middle_at = a_rim.shape[0]

    def base_pass(start, count, pieces, begin, end):
        rows = pl.ds(start, count)
        product = across([vert[rows, 2 * b * LANE : (2 * b + 3) * LANE] for b in range(begin, end)], g_base[...])
        for b in range(begin, end):
            at = (b - begin) * count
            for first_row, size in pieces:
                base[pl.ds(first_row, size), b * LANE : (b + 1) * LANE] = product[at : at + size]
                at += size

    def own_pass(begin, end):
        vert[:, begin * LANE : end * LANE] = jnp.dot(
            a_fine[...], own_operand(ext, keep, begin, end), preferred_element_type=F32
        )

    base_rows = 2 * base_edge

    def rim_pass(rows, begin, end):
        vert[rows, begin * LANE : end * LANE] += jnp.dot(
            a_rim[rows, :], rim_operand(rim_in_pair, keep, begin, end), preferred_element_type=F32
        )

    rim_in_pair = [above, below]
    start_at = [0] + ready_at[:-1]
    base_at = [0] + [(ready - 1) // 2 for ready in ready_at]
    block_at = [0] + [ready - 1 for ready in ready_at[:-1]] + [tiles + 1]
    for j in range(chunks):
        own_pass(start_at[j], ready_at[j])
        base_pass(
            middle_at, half_rows - 2 * base_edge, [(base_edge, half_rows - 2 * base_edge)], base_at[j], base_at[j + 1]
        )
        horizontal_pass(
            vert, g_level, lev, middle_at + half_rows - 2 * base_edge, middle_rows,
            [(EDGE, middle_rows)], high_rows, block_at[j], block_at[j + 1],
        )

    @pl.when(has_up)
    def _():
        to_down_corner.wait_recv()

    @pl.when(has_down)
    def _():
        to_up_corner.wait_recv()

    sends, ups, downs = [], [], []
    for j in range(chunks):

        @pl.when(has_up)
        def _():
            to_down[j].wait_recv()

        @pl.when(has_down)
        def _():
            to_up[j].wait_recv()

        rim_pass(slice(0, base_rows), start_at[j], ready_at[j])
        base_pass(
            0, base_rows, [(0, base_edge), (half_rows - base_edge, base_edge)], base_at[j], base_at[j + 1]
        )

        columns = (base_at[j + 1] - base_at[j]) * LANE
        near = pl.ds(base_at[j] * LANE, columns)
        mine = pl.ds(pl.multiple_of(c * half_cols + base_at[j] * LANE, LANE), columns)
        crim_out[0, :, near] = packed(base[0:RIM, near], NEED, slot < NEED)
        crim_out[1, :, near] = packed(base[half_rows - RIM : half_rows, near], SPARE, slot >= SPARE)
        up = remote(
            crim_out.at[0, :, near], crim.at[:, mine], csend.at[3 * j], crecv.at[3 * j + c], r - 1, 1
        )
        down = remote(
            crim_out.at[1, :, near], crim.at[:, mine], csend.at[3 * j + 1], crecv.at[3 * j + c], r + 1, 0
        )
        pair = remote(base.at[:, near], cext.at[:, mine], csend.at[3 * j + 2], crecv.at[3 * j + 2], r, other)
        ups.append(up)
        downs.append(down)
        sends.append(pair)

        @pl.when(has_up)
        def _():
            up.start()

        @pl.when(has_down)
        def _():
            down.start()

        pair.start()
        cext[:, mine] = base[:, near]

    for j in range(chunks):
        rim_pass(slice(base_rows, middle_at), start_at[j], ready_at[j])

    for j in range(chunks):
        horizontal_pass(
            vert, g_level, lev, base_rows, edge_rows, edge_pieces, high_rows, block_at[j], block_at[j + 1]
        )

    edge_keep = jnp.where(lane == jnp.where(c == 0, 0, LANE - 1), 1.0, 0.0).astype(F32)
    responses(
        lev, diff, tile_rows, tiles + 1, 20.0, 5000.0,
        row_mask(tile_rows, has_up, has_down), edge_keep, dog_fine, hess_fine,
    )

    for send in sends:
        send.wait_recv()

    @pl.when(jnp.logical_or(c == 1, has_up))
    def _():
        @pl.when(jnp.logical_or(c == 0, has_down))
        def _():
            for j in range(chunks):
                for index in range(2):
                    pltpu.make_async_remote_copy(
                        src_ref=ups[j].src_ref, dst_ref=ups[j].dst_ref,
                        send_sem=csend.at[3 * j], recv_sem=crecv.at[3 * j + index],
                        device_id={"row": r, "col": other}, device_id_type=MESH,
                    ).wait_recv()

    @pl.when(has_down)
    def _():
        to_down_corner.wait_send()
        for send in to_down + downs:
            send.wait_send()

    @pl.when(has_up)
    def _():
        to_up_corner.wait_send()
        for send in to_up + ups:
            send.wait_send()

    for send in sends:
        send.wait_send()


def finish(
    rows_total, dog_near, hess_near, cext, crim, a_coarse, g_level,
    dog_fine, hess_fine, dog_coarse, hess_coarse,
    vert, lev, diff, dog, hess, sem,
):
    strip = cext.shape[0] // 2
    tiles = cext.shape[1] // LANE - 1
    r = lax.axis_index("row")
    c = lax.axis_index("col")
    fine = [
        pltpu.make_async_copy(dog_near, dog_fine, sem.at[0]),
        pltpu.make_async_copy(hess_near, hess_fine, sem.at[1]),
    ]
    for copy in fine:
        copy.start()
    for begin in range(0, tiles, CHUNK):
        end = begin + CHUNK + (1 if begin + CHUNK == tiles else 0)
        operand = jnp.concatenate(
            [own_operand(cext, None, begin, end), rim_operand([crim], None, begin, end)], axis=0
        )
        vert[:, begin * LANE : end * LANE] = jnp.dot(a_coarse[c], operand, preferred_element_type=F32)
    horizontal_pass(vert, g_level, lev, 0, strip + RING, [(0, strip + RING)], strip + RING, 0, tiles)
    responses(
        lev, diff, strip, tiles, 80.0, 200000.0,
        row_mask(strip, jnp.logical_or(r > 0, c == 1), jnp.logical_or(r < rows_total - 1, c == 0)),
        None, dog, hess,
    )
    coarse = [
        pltpu.make_async_copy(dog, dog_coarse, sem.at[2]),
        pltpu.make_async_copy(hess, hess_coarse, sem.at[3]),
    ]
    for copy in coarse:
        copy.start()
    for copy in fine + coarse:
        copy.wait()


def solution(mesh):
    rows_total = mesh.shape["row"]

    def local(image):
        tile_rows, tile_cols = image.shape
        strip = tile_rows // 4
        tiles = tile_cols // LANE
        base_edge = EDGE // 2
        half_rows = tile_rows // 2
        numbers = np.arange(half_rows, dtype=np.float64)
        level_rows = ring_rows(tile_rows)

        def fine_matrix(base_rows, rows, inputs):
            matrix = np.concatenate(
                [vertical_matrix(2.0 * base_rows, inputs, SIGMAS[4])]
                + [vertical_matrix(rows, inputs, s) for s in SIGMAS]
            )
            return pad_rows(matrix, 16)

        def edges_of(x, edge, length):
            return np.concatenate([x[:edge], x[length - edge :]])

        fine_in = np.arange(tile_rows, dtype=np.float64)
        edge_out = edges_of(numbers, base_edge, half_rows), edges_of(level_rows, EDGE, tile_rows)
        middle_out = numbers[base_edge : half_rows - base_edge], level_rows[EDGE : tile_rows - EDGE]
        a_fine = own_weights(np.concatenate([fine_matrix(*edge_out, fine_in), fine_matrix(*middle_out, fine_in)]))
        a_rim = rim_weights(fine_matrix(*edge_out, rim_inputs(tile_rows)))
        coarse_out = [strip * c + ring_rows(strip) for c in range(2)]
        coarse_rim = [rim_inputs(2 * strip)[:RIM], rim_inputs(2 * strip)[RIM:]]

        def coarse_matrix(c, inputs):
            return pad_rows(np.concatenate([vertical_matrix(coarse_out[c], inputs, s) for s in SIGMAS]), 16)

        a_coarse = np.stack(
            [
                np.concatenate(
                    [
                        own_weights(coarse_matrix(c, np.arange(2 * strip, dtype=np.float64))),
                        rim_weights(coarse_matrix(c, coarse_rim[c])),
                    ],
                    axis=1,
                )
                for c in range(2)
            ]
        )
        span = np.arange(2 * LANE, dtype=np.float64)[:, None] - HALF
        g_level = np.stack(
            [column_weights(taps_at(s, span - np.arange(LANE)[None, :])) for s in SIGMAS]
        )
        wider = np.arange(3 * LANE, dtype=np.float64)[:, None] - HALF
        g_base = column_weights(taps_at(SIGMAS[4], wider - 2.0 * np.arange(LANE)[None, :]))

        vmem = pl.BlockSpec(memory_space=pltpu.VMEM)
        ring = tile_rows + 8
        wide = tile_cols + LANE
        chunks = tiles // CHUNK
        hbm = pl.BlockSpec(memory_space=pltpu.HBM)
        near = pl.pallas_call(
            functools.partial(kernel, rows_total),
            out_shape=(
                pltpu.VMEM((4, tile_rows, tile_cols), BF),
                pltpu.VMEM((2, tile_rows, tile_cols), BF),
                pltpu.VMEM((2 * strip, wide), F32),
                pltpu.VMEM((RIM, wide), BF),
                pltpu.VMEM(a_coarse.shape, BF),
                pltpu.VMEM(g_level.shape, BF),
            ),
            in_specs=[hbm] * 6,
            out_specs=(vmem,) * 6,
            scratch_shapes=[
                pltpu.VMEM((tile_rows, wide), F32),
                pltpu.VMEM((2, RIM, tile_cols), BF),
                pltpu.VMEM((2, RIM, wide), BF),
                pltpu.VMEM((2, RIM, tile_cols // 2), BF),
                pltpu.VMEM((a_fine.shape[0], wide), F32),
                pltpu.VMEM((LEVELS, (tiles + 1) * ring, LANE), F32),
                pltpu.VMEM((2, (tiles + 1) * ring, LANE), F32),
                pltpu.VMEM((tile_rows // 2, tile_cols // 2), F32),
                pltpu.VMEM(a_fine.shape, BF),
                pltpu.VMEM(a_rim.shape, BF),
                pltpu.VMEM(g_base.shape, BF),
                pltpu.SemaphoreType.DMA((6,)),
                pltpu.SemaphoreType.DMA((2 * chunks + 3,)),
                pltpu.SemaphoreType.DMA((2 * chunks + 3,)),
                pltpu.SemaphoreType.DMA((3 * chunks,)),
                pltpu.SemaphoreType.DMA((3 * chunks,)),
            ],
            compiler_params=pltpu.CompilerParams(
                collective_id=0, has_side_effects=True, vmem_limit_bytes=32000000
            ),
        )(*[pltpu.with_memory_space_constraint(x, pltpu.HBM) for x in (image, a_fine, a_rim, a_coarse, g_level, g_base)])
        coarse_ring = strip + 8
        return pl.pallas_call(
            functools.partial(finish, rows_total),
            out_shape=(
                jax.ShapeDtypeStruct((4, tile_rows, tile_cols), BF),
                jax.ShapeDtypeStruct((2, tile_rows, tile_cols), BF),
                jax.ShapeDtypeStruct((4, strip, tile_cols), BF),
                jax.ShapeDtypeStruct((2, strip, tile_cols), BF),
            ),
            in_specs=[vmem] * 6,
            out_specs=(hbm,) * 4,
            scratch_shapes=[
                pltpu.VMEM((a_coarse.shape[1], wide), F32),
                pltpu.VMEM((LEVELS, tiles * coarse_ring, LANE), F32),
                pltpu.VMEM((2, (tiles + 1) * coarse_ring, LANE), F32),
                pltpu.VMEM((4, strip, tile_cols), BF),
                pltpu.VMEM((2, strip, tile_cols), BF),
                pltpu.SemaphoreType.DMA((4,)),
            ],
            compiler_params=pltpu.CompilerParams(vmem_limit_bytes=32000000),
        )(*near)

    return jax.shard_map(
        local,
        mesh=mesh,
        in_specs=(P(("slab", "row"), "col"),),
        out_specs=(
            P(None, ("slab", "row"), "col"),
            P(None, ("slab", "row"), "col"),
            P(None, ("slab", "row", "col"), None),
            P(None, ("slab", "row", "col"), None),
        ),
        check_vma=False,
    )
```
